512 devices in a mesh: grid: 8 (over x, core), samp: 64 (over z, y).
Axes of the slice: x: 4, y: 4, z: 16, core: 2. Of those that a mesh axis runs over, the one named last changes fastest.
Arguments:
- summary: bfloat16 [131072, 1024], P('samp'), may hold values from -10 to 10
- kernel: bfloat16 [1024, 4096], P(None, 'grid'), may hold values from -1 to 1
- grid_offset: float32 [4096], P('grid'), may hold values from -130 to 130
- log_prior: float32 [131072], P('samp'), may hold values from -6 to 6
- tile_event: int32 [1024], P('samp'), may hold values from 0 to 63, as said below
- tile_live: int32 [1024], P('samp'), may hold values from 2 to 128
Outputs:
- log_evidence: float32 [64, 4096], P('samp', 'grid')
- ess_fraction: float32 [64, 4096], P('samp', 'grid')
- log_posterior: float32 [4096], P('grid')
The draws below stay inside these ranges and needn't reach their ends.
Inputs may be any that keep to these rules, and one draw needn't show every extreme that they name: `tile_event`: every event owns at least one tile.
All inputs are finite; a program needn't handle non-finite values.
Results may differ from the reference program's by a relative error of at most 0.0003.
Values sent between devices are 32-bit elements; how exact they have to be, the bound alone decides.
A program may use at most 64 MiB of HBM per device.

```python
import jax
import jax.numpy as jnp
from jax import lax

BINS = 1024
GRID = 4096
EVENTS = 64
TILE = 128
ROWS_DEV = 2048
TILES_DEV = 16
SAMPLES = 131072
TILES = 1024
N_SAMP = 64


def kernel_table(key):
    raw = jax.random.normal(jax.random.fold_in(key, 101), (BINS, GRID), jnp.float32)
    return jnp.clip(raw, -4.0, 4.0) / jnp.sqrt(jnp.float32(BINS))


def draw_kernel(key, part):
    return kernel_table(key).astype(jnp.bfloat16)


def draw_summary(key, part):
    table = kernel_table(key)
    noise = jnp.clip(jax.random.normal(jax.random.fold_in(key, 202), (SAMPLES, BINS), jnp.float32), -6.0, 6.0)
    column = jax.random.randint(jax.random.fold_in(key, 303), (TILES,), 0, GRID, dtype=jnp.int32)
    strength = jnp.exp(jax.random.uniform(jax.random.fold_in(key, 404), (TILES,), jnp.float32, jnp.log(0.5), jnp.log(10.0)))
    chosen = jnp.take(table, column, axis=1).T
    pattern = jnp.where(chosen >= 0.0, jnp.float32(1.0), jnp.float32(-1.0))
    top_score = strength * jnp.sum(jnp.abs(chosen), axis=1)
    lower = 1.0 - 2.0 / top_score
    row_zero = strength[:, None] * pattern
    row_one = row_zero * lower[:, None]
    shaped = noise.reshape(TILES, TILE, BINS)
    shaped = shaped.at[:, 0, :].set(row_zero)
    shaped = shaped.at[:, 1, :].set(row_one)
    return shaped.reshape(SAMPLES, BINS).astype(jnp.bfloat16)


def draw_grid_offset(key, part):
    return jnp.clip(jax.random.normal(key, (GRID,), jnp.float32), -6.0, 6.0)


def draw_tile_event(key, part):
    first_key = jax.random.fold_in(key, 11)
    second_key = jax.random.fold_in(key, 23)
    extra = jax.random.randint(first_key, (TILES - EVENTS,), 0, EVENTS, dtype=jnp.int32)
    listing = jnp.concatenate([jnp.arange(EVENTS, dtype=jnp.int32), extra])
    return jax.random.permutation(second_key, listing).astype(jnp.int32)


def touch_ends(array, own_key, low, high):
    spot = [jax.random.randint(jax.random.fold_in(own_key, axis), (), 0, length) for axis, length in enumerate(array.shape)]
    widest = array.shape.index(max(array.shape))
    beside = spot[:widest] + [(spot[widest] + 1) % array.shape[widest]] + spot[widest + 1:]
    return array.at[tuple(spot)].set(low).at[tuple(beside)].set(high)


def level_of(key, extent, split, smallest, high):
    level, own = 1.0, jax.random.fold_in(key, 6)
    for dim, parts in split:
        heights = jnp.exp(jax.random.uniform(jax.random.fold_in(own, dim), (parts,), jnp.float32, smallest / len(split), high / len(split)))
        level = level * jnp.repeat(heights, extent[dim] // parts).reshape([-1 if axis == dim else 1 for axis in range(len(extent))])
    return level


def scatter_about(key, shape, scale, reach, split=(), kind=jnp.bfloat16):
    loudness = level_of(key, shape, split, -0.22, 0.18) if split else 1.0
    entries = jax.random.normal(key, shape, jnp.float32) * scale * loudness
    return jnp.minimum(jnp.maximum(entries, -reach), reach).astype(kind)


def setup_inputs(seed: int = 0) -> dict:
    splits = jax.random.split(jax.random.key(seed), 7)
    summary = draw_summary(jax.random.fold_in(splits[6], 71), 0)
    kernel = draw_kernel(jax.random.fold_in(splits[6], 71), 0)
    grid_offset = draw_grid_offset(jax.random.fold_in(splits[6], 71), 0)
    log_prior = scatter_about(splits[3], (SAMPLES,), 1.0, 6.0, ((0, 64),), jnp.float32)
    tile_event = draw_tile_event(jax.random.fold_in(splits[6], 71), 0)
    tile_live = touch_ends(jax.random.randint(splits[5], (TILES,), 2, TILE + 1), jax.random.fold_in(splits[5], 1), 2, TILE).astype(jnp.int32)
    return {"summary": summary, "kernel": kernel, "grid_offset": grid_offset, "log_prior": log_prior, "tile_event": tile_event, "tile_live": tile_live}


def reference(summary, kernel, grid_offset, log_prior, tile_event, tile_live):
    def block_stats(packed):
        block_rows, block_prior, block_live = packed
        scores = jnp.dot(block_rows, kernel, preferred_element_type=jnp.float32)
        scores = scores + grid_offset[None, :] - block_prior[:, None]
        scores = scores.reshape(TILES_DEV, TILE, GRID)
        is_live = lax.broadcasted_iota(jnp.int32, (TILES_DEV, TILE), 1) < block_live[:, None]
        masked = jnp.where(is_live[:, :, None], scores, jnp.float32(-1e30))
        tile_max = jnp.max(masked, axis=1)
        shifted = jnp.exp(masked - tile_max[:, None, :])
        return tile_max, jnp.sum(shifted, axis=1), jnp.sum(shifted * shifted, axis=1)

    tile_max, tile_first, tile_second = lax.map(block_stats, (summary.reshape(N_SAMP, ROWS_DEV, BINS), log_prior.reshape(N_SAMP, ROWS_DEV), tile_live.reshape(N_SAMP, TILES_DEV)))
    tile_max = tile_max.reshape(TILES, GRID)
    tile_first = tile_first.reshape(TILES, GRID)
    tile_second = tile_second.reshape(TILES, GRID)

    def event_stats(event_id):
        member = tile_event == event_id
        event_max = jnp.max(jnp.where(member[:, None], tile_max, jnp.float32(-1e30)), axis=0)
        factor = jnp.exp(tile_max - event_max[None, :])
        first_sum = jnp.sum(jnp.where(member[:, None], tile_first * factor, jnp.float32(0.0)), axis=0)
        second_sum = jnp.sum(jnp.where(member[:, None], tile_second * factor * factor, jnp.float32(0.0)), axis=0)
        live_count = jnp.sum(jnp.where(member, tile_live, 0)).astype(jnp.float32)
        evidence = event_max + jnp.log(first_sum) - jnp.log(live_count)
        return evidence, first_sum * first_sum / (second_sum * live_count)

    log_evidence, ess_fraction = lax.map(event_stats, jnp.arange(EVENTS, dtype=jnp.int32))
    loglik = jnp.sum(log_evidence, axis=0) / jnp.float32(EVENTS)
    grid_top = jnp.max(loglik)
    log_norm = grid_top + jnp.log(jnp.sum(jnp.exp(loglik - grid_top)))
    return log_evidence, ess_fraction, loglik - log_norm
```

```python
import jax
import jax.numpy as jnp
from jax import lax
from jax.experimental import pallas as pl
from jax.experimental.pallas import tpu as pltpu
from jax.sharding import PartitionSpec as P

EVENTS = 64
NX, NC, NY, NZ = 4, 2, 4, 16
NG = NX * NC
TILE = 128
LANE = 128
NJ = 4
TILES = 16
GROUPS = 4
PER = TILES // GROUPS
BIG = -1e30
LOG2E = 1.4426950408889634
MESH = pl.DeviceIdType.MESH


def at_device(grid, samp):
    return (grid, samp)


def kernel(
    summary, weight, prior, offset, event, live,
    evidence_out, ess_out, posterior_out,
    x_buf, w_buf, scores, prior_buf, offset_buf,
    yid, yst, zsend, zrecv, csend, crecv, lbuf, vbuf,
    in_sem, y_send, y_recv, id_send, id_recv, z_send, z_recv, c_send, c_recv,
    l_send, l_recv, v_send, v_recv,
):
    gi, si = lax.axis_index("grid"), lax.axis_index("samp")
    x, c = gi // NC, lax.rem(gi, NC)
    z, y = si // NY, lax.rem(si, NY)
    rows = x_buf.shape[0]
    chunk = rows // GROUPS

    y_peers = [(gi, z * NY + lax.rem(y + d, NY)) for d in range(1, NY)]
    z_index = [lax.rem(z + d, NZ) for d in range(1, NZ)]
    z_peers = [(gi, zi * NY + y) for zi in z_index]
    v_peers = []
    for dx in range(NX):
        for dc in range(NC):
            for dy in range(NY):
                if dx or dc or dy:
                    grid = lax.rem(x + dx, NX) * NC + lax.rem(c + dc, NC)
                    v_peers.append((grid, z * NY + lax.rem(y + dy, NY)))

    copies = [
        pltpu.make_async_copy(weight, w_buf, in_sem.at[0]),
        pltpu.make_async_copy(prior, prior_buf, in_sem.at[1]),
        pltpu.make_async_copy(offset, offset_buf, in_sem.at[2]),
    ]
    for g in range(GROUPS):
        part = pl.ds(g * chunk, chunk)
        copies.append(pltpu.make_async_copy(summary.at[part], x_buf.at[part], in_sem.at[3 + g]))
    for copy in copies:
        copy.start()

    barrier = pltpu.get_barrier_semaphore()
    greeted = z_peers + v_peers
    for peer in greeted:
        pl.semaphore_signal(barrier, inc=1, device_id=peer, device_id_type=MESH)

    for t in range(TILES):
        yid[y, 0, t : t + 1, :] = jnp.full((1, LANE), event[t].astype(jnp.float32))
        yid[y, 1, t : t + 1, :] = jnp.full((1, LANE), live[t].astype(jnp.float32))

    lane = lax.broadcasted_iota(jnp.int32, (1, LANE), 1)

    def dot(g):
        copies[3 + g].wait()
        scores[g % 2] = jnp.dot(
            x_buf[g * chunk : (g + 1) * chunk, :], w_buf[...], preferred_element_type=jnp.float32
        )

    def stats(g):
        for i in range(PER):
            t = g * PER + i
            add = jnp.where(lane < live[t], -prior_buf[t : t + 1, :], BIG)
            add = jnp.transpose(jnp.broadcast_to(add, (LANE, LANE)))
            for j in range(NJ):
                v = scores[g % 2, i * TILE : (i + 1) * TILE, j * LANE : (j + 1) * LANE] + add
                top = jnp.max(v, axis=0, keepdims=True)
                p = jnp.exp2((v - top) * LOG2E)
                first = jnp.sum(p, axis=0, keepdims=True)
                second = jnp.sum(p * p, axis=0, keepdims=True)
                at = i * NJ + j
                yst[g, y, 0, at : at + 1, :] = top + jnp.log(first)
                yst[g, y, 1, at : at + 1, :] = second / (first * first)

    copies[0].wait()
    copies[1].wait()
    dot(0)
    for g in range(1, GROUPS):
        dot(g)
        stats(g - 1)
    stats(GROUPS - 1)

    pl.semaphore_wait(barrier, len(greeted))

    sends = []

    def remote(src, dst, send_sem, recv_sem, peer):
        copy = pltpu.make_async_remote_copy(
            src_ref=src, dst_ref=dst, send_sem=send_sem, recv_sem=recv_sem,
            device_id=peer, device_id_type=MESH,
        )
        copy.start()

    def arrived(ref, send_sem, recv_sem):
        copy = pltpu.make_async_remote_copy(
            src_ref=ref, dst_ref=ref, send_sem=send_sem, recv_sem=recv_sem,
            device_id=y_peers[0], device_id_type=MESH,
        )
        copy.wait_recv()
        sends.append(copy)

    for peer in y_peers:
        remote(yid.at[y], yid.at[y], id_send, id_recv, peer)
    for g in range(GROUPS):
        for peer in y_peers:
            remote(yst.at[g, y], yst.at[g, y], y_send.at[g], y_recv.at[g], peer)

    arrived(yid.at[pl.ds(0, NY - 1)], id_send, id_recv)
    mine = lax.broadcasted_iota(jnp.int32, (NZ, LANE), 0) * NY + y
    mine = mine.astype(jnp.float32)

    def member(s, t):
        return jnp.broadcast_to(yid[s, 0, t : t + 1, :], (NZ, LANE)) == mine

    count = jnp.zeros((NZ, LANE), jnp.float32)
    for s in range(NY):
        for t in range(TILES):
            count += jnp.where(member(s, t), yid[s, 1, t : t + 1, :], 0.0)
    for k in range(NZ):
        csend[k] = count[k : k + 1, :]
    crecv[z] = csend[z]
    for zi, peer in zip(z_index, z_peers):
        remote(csend.at[zi], crecv.at[z], c_send, c_recv, peer)

    for g in range(GROUPS):
        arrived(yst.at[g, pl.ds(0, NY - 1)], y_send.at[g], y_recv.at[g])
    order = [(s, g, i) for g in range(GROUPS) for s in range(NY) for i in range(PER)]
    for j in range(NJ):
        top = jnp.full((NZ, LANE), BIG, jnp.float32)
        for s, g, i in order:
            at = i * NJ + j
            row = yst[g, s, 0, at : at + 1, :]
            top = jnp.maximum(top, jnp.where(member(s, g * PER + i), row, BIG))
        first = jnp.zeros((NZ, LANE), jnp.float32)
        second = jnp.zeros((NZ, LANE), jnp.float32)
        for s, g, i in order:
            at = i * NJ + j
            row = jnp.where(member(s, g * PER + i), yst[g, s, 0, at : at + 1, :], BIG)
            w = jnp.exp2((row - top) * LOG2E)
            first += w
            second += w * w * yst[g, s, 1, at : at + 1, :]
        zsend[pl.ds(j, NZ, stride=8), :] = top + jnp.log(first)
        zsend[pl.ds(NJ + j, NZ, stride=8), :] = second / (first * first)

    def block(index):
        return pl.ds(pl.multiple_of(index * 8, 8), 8)

    for zi, peer in zip(z_index, z_peers):
        remote(zsend.at[block(zi)], zrecv.at[block(z)], z_send, z_recv, peer)
    zrecv[block(z), :] = zsend[block(z), :]

    arrived(crecv.at[pl.ds(0, NZ - 1)], c_send, c_recv)
    total = crecv[0]
    for k in range(1, NZ):
        total += crecv[k]
    copies[2].wait()
    arrived(zrecv.at[pl.ds(0, 8 * (NZ - 1))], z_send, z_recv)
    top = zrecv[0:NJ, :]
    for k in range(1, NZ):
        top = jnp.maximum(top, zrecv[8 * k : 8 * k + NJ, :])
    first = jnp.zeros((NJ, LANE), jnp.float32)
    second = jnp.zeros((NJ, LANE), jnp.float32)
    for k in range(NZ):
        w = jnp.exp2((zrecv[8 * k : 8 * k + NJ, :] - top) * LOG2E)
        first += w
        second += w * w * zrecv[8 * k + NJ : 8 * k + 8, :]
    evidence = (top + jnp.log(first)) + offset_buf[...] - jnp.log(total)
    lbuf[z] = evidence
    for peer in z_peers:
        remote(lbuf.at[z], lbuf.at[z], l_send, l_recv, peer)
    evidence_out[...] = evidence
    ess_out[...] = first * first / (second * total)

    arrived(lbuf.at[pl.ds(0, NZ - 1)], l_send, l_recv)
    partial = lbuf[0]
    for k in range(1, NZ):
        partial += lbuf[k]
    vbuf[gi * NY + y] = partial
    for peer in v_peers:
        remote(vbuf.at[gi * NY + y], vbuf.at[gi * NY + y], v_send, v_recv, peer)
    arrived(vbuf.at[pl.ds(0, NG * NY - 1)], v_send, v_recv)

    def loglik(index):
        value = vbuf[index * NY]
        for k in range(1, NY):
            value += vbuf[index * NY + k]
        return value * (1.0 / EVENTS)

    lines = [loglik(k) for k in range(NG)]
    best = lines[0]
    for line in lines[1:]:
        best = jnp.maximum(best, line)
    best = jnp.max(best)
    mass = jnp.zeros((NJ, LANE), jnp.float32)
    for line in lines:
        mass += jnp.exp2((line - best) * LOG2E)
    mass = jnp.sum(mass)
    norm = best + jnp.log(jnp.full((NJ, LANE), mass))
    posterior_out[...] = loglik(gi) - norm

    for copy in sends:
        copy.wait_send()


def body(summary, weight, offset, prior, event, live):
    rows, bins = summary.shape
    cols = weight.shape[1]
    dma, vmem = pltpu.SemaphoreType.DMA, pltpu.VMEM
    f32 = jnp.float32
    small = jax.ShapeDtypeStruct((NJ, LANE), f32)
    hbm = pl.BlockSpec(memory_space=pltpu.HBM)
    smem = pl.BlockSpec(memory_space=pltpu.SMEM)
    outs = pl.pallas_call(
        kernel,
        name="reweight",
        out_shape=(small, small, small),
        in_specs=[hbm, hbm, hbm, hbm, smem, smem],
        out_specs=(pl.BlockSpec(memory_space=pltpu.VMEM),) * 3,
        scratch_shapes=[
            vmem((rows, bins), jnp.bfloat16),
            vmem((bins, cols), jnp.bfloat16),
            vmem((2, rows // GROUPS, cols), f32),
            vmem((TILES, LANE), f32),
            vmem((NJ, LANE), f32),
            vmem((NY, 2, TILES, LANE), f32),
            vmem((GROUPS, NY, 2, PER * NJ, LANE), f32),
            vmem((NZ * 8, LANE), f32),
            vmem((NZ * 8, LANE), f32),
            vmem((NZ, 1, LANE), f32),
            vmem((NZ, 1, LANE), f32),
            vmem((NZ, NJ, LANE), f32),
            vmem((NG * NY, NJ, LANE), f32),
            dma((3 + GROUPS,)),
            dma((GROUPS,)),
            dma((GROUPS,)),
            dma, dma, dma, dma, dma, dma, dma, dma, dma, dma,
        ],
        compiler_params=pltpu.CompilerParams(
            collective_id=0, has_side_effects=True, vmem_limit_bytes=32 * 1024 * 1024
        ),
        cost_estimate=pl.CostEstimate(
            flops=2 * rows * bins * cols, bytes_accessed=2 * rows * bins, transcendentals=rows * cols
        ),
    )(summary, weight, prior.reshape(TILES, LANE), offset.reshape(NJ, LANE), event, live)
    evidence, ess, posterior = outs
    return evidence.reshape(1, cols), ess.reshape(1, cols), posterior.reshape(cols)


def solution(mesh):
    in_specs = (P("samp", None), P(None, "grid"), P("grid"), P("samp"), P("samp"), P("samp"))
    out_specs = (P("samp", "grid"), P("samp", "grid"), P("grid"))
    return jax.shard_map(body, mesh=mesh, in_specs=in_specs, out_specs=out_specs, check_vma=False)
```

```python
import jax
import jax.numpy as jnp
from jax import lax
from jax.experimental import pallas as pl
from jax.experimental.pallas import tpu as pltpu
from jax.sharding import PartitionSpec as P

EVENTS = 64
NX, NC, NY, NZ = 4, 2, 4, 16
NG = NX * NC
TILE = 128
LANE = 128
NJ = 4
TILES = 16
GROUPS = 4
PER = TILES // GROUPS
BIG = -1e30
LOG2E = 1.4426950408889634
MESH = pl.DeviceIdType.MESH
RELAY = (1, 2, 4)


def at_device(grid, samp):
    return (grid, samp)


def kernel(
    summary, weight, prior, offset, event, live,
    evidence_out, ess_out, posterior_out,
    x_buf, w_buf, scores, prior_buf, offset_buf,
    yid, yst, held, zsend, zrecv, csend, crecv, lbuf, vbuf,
    in_sem, y_send, y_recv, id_send, id_recv, z_send, z_recv, c_send, c_recv,
    l_send, l_recv, v_send, v_recv, known,
):
    gi, si = lax.axis_index("grid"), lax.axis_index("samp")
    x, c = gi // NC, lax.rem(gi, NC)
    z, y = si // NY, lax.rem(si, NY)
    rows = x_buf.shape[0]
    chunk = rows // GROUPS

    y_peers = [(gi, z * NY + lax.rem(y + d, NY)) for d in range(1, NY)]
    z_index = [lax.rem(z + d, NZ) for d in range(1, NZ)]
    z_peers = [(gi, zi * NY + y) for zi in z_index]
    v_peers = []
    for dx in range(NX):
        for dc in range(NC):
            for dy in range(NY):
                if dx or dc or dy:
                    grid = lax.rem(x + dx, NX) * NC + lax.rem(c + dc, NC)
                    v_peers.append((grid, z * NY + lax.rem(y + dy, NY)))

    copies = [
        pltpu.make_async_copy(weight, w_buf, in_sem.at[0]),
        pltpu.make_async_copy(prior, prior_buf, in_sem.at[1]),
        pltpu.make_async_copy(offset, offset_buf, in_sem.at[2]),
    ]
    for g in range(GROUPS):
        part = pl.ds(g * chunk, chunk)
        copies.append(pltpu.make_async_copy(summary.at[part], x_buf.at[part], in_sem.at[3 + g]))
    for copy in copies:
        copy.start()

    def beside(d):
        return [(gi, lax.rem(z + k, NZ) * NY + y) for k in (d, NZ - d)]

    grid_peers = []
    for dx in range(NX):
        for dc in range(NC):
            if dx or dc:
                grid_peers.append((lax.rem(x + dx, NX) * NC + lax.rem(c + dc, NC), si))
    near = y_peers + grid_peers + beside(1)
    barrier = pltpu.get_barrier_semaphore()
    for peer in near:
        pl.semaphore_signal(barrier, inc=1, device_id=peer, device_id_type=MESH)

    def tell(k):
        for peer in beside(RELAY[k]):
            pl.semaphore_signal(known.at[k], inc=1, device_id=peer, device_id_type=MESH)

    def heard(k):
        pl.semaphore_wait(known.at[k], 2)

    for t in range(TILES):
        yid[y, 0, t : t + 1, :] = jnp.full((1, LANE), event[t].astype(jnp.float32))
        yid[y, 1, t : t + 1, :] = jnp.full((1, LANE), live[t].astype(jnp.float32))

    lane = lax.broadcasted_iota(jnp.int32, (1, LANE), 1)

    def dot(g):
        copies[3 + g].wait()
        scores[g % 2] = jnp.dot(
            x_buf[g * chunk : (g + 1) * chunk, :], w_buf[...], preferred_element_type=jnp.float32
        )

    def stats(g):
        for i in range(PER):
            t = g * PER + i
            add = jnp.where(lane < live[t], -prior_buf[t : t + 1, :], BIG)
            add = jnp.transpose(jnp.broadcast_to(add, (LANE, LANE)))
            for j in range(NJ):
                v = scores[g % 2, i * TILE : (i + 1) * TILE, j * LANE : (j + 1) * LANE] + add
                top = jnp.max(v, axis=0, keepdims=True)
                p = jnp.exp2((v - top) * LOG2E)
                first = jnp.sum(p, axis=0, keepdims=True)
                second = jnp.sum(p * p, axis=0, keepdims=True)
                at = i * NJ + j
                yst[g, y, 0, at : at + 1, :] = top + jnp.log(first)
                yst[g, y, 1, at : at + 1, :] = second / (first * first)

    sends = []

    def remote(src, dst, send_sem, recv_sem, peer):
        copy = pltpu.make_async_remote_copy(
            src_ref=src, dst_ref=dst, send_sem=send_sem, recv_sem=recv_sem,
            device_id=peer, device_id_type=MESH,
        )
        copy.start()

    def arrived(ref, send_sem, recv_sem):
        copy = pltpu.make_async_remote_copy(
            src_ref=ref, dst_ref=ref, send_sem=send_sem, recv_sem=recv_sem,
            device_id=y_peers[0], device_id_type=MESH,
        )
        copy.wait_recv()
        sends.append(copy)

    def send_stats(g):
        for peer in y_peers:
            remote(yst.at[g, y], yst.at[g, y], y_send.at[g], y_recv.at[g], peer)

    def got_stats(g):
        arrived(yst.at[g, pl.ds(0, NY - 1)], y_send.at[g], y_recv.at[g])

    pl.semaphore_wait(barrier, len(near))
    tell(0)
    for peer in y_peers:
        remote(yid.at[y], yid.at[y], id_send, id_recv, peer)
    copies[0].wait()
    copies[1].wait()
    dot(0)
    for g in range(1, GROUPS):
        dot(g)
        stats(g - 1)
        send_stats(g - 1)
        if g == 1:
            heard(0)
            tell(1)
    stats(GROUPS - 1)
    send_stats(GROUPS - 1)
    heard(1)
    tell(2)

    arrived(yid.at[pl.ds(0, NY - 1)], id_send, id_recv)
    mine = lax.broadcasted_iota(jnp.int32, (NZ, LANE), 0) * NY + y
    mine = mine.astype(jnp.float32)

    def member(s, t):
        return jnp.broadcast_to(yid[s, 0, t : t + 1, :], (NZ, LANE)) == mine

    count = jnp.zeros((NZ, LANE), jnp.float32)
    for s in range(NY):
        for t in range(TILES):
            count += jnp.where(member(s, t), yid[s, 1, t : t + 1, :], 0.0)
    for k in range(NZ):
        csend[k] = count[k : k + 1, :]
    crecv[z] = csend[z]

    def rows_of(groups):
        return [(s, g, i) for g in groups for s in range(NY) for i in range(PER)]

    def chosen(j, s, g, i):
        at = i * NJ + j
        return jnp.where(member(s, g * PER + i), yst[g, s, 0, at : at + 1, :], BIG)

    def merged(j, order, top, first, second):
        high = top
        for entry in order:
            high = jnp.maximum(high, chosen(j, *entry))
        keep = jnp.exp2((top - high) * LOG2E)
        first, second = first * keep, second * (keep * keep)
        for s, g, i in order:
            at = i * NJ + j
            w = jnp.exp2((chosen(j, s, g, i) - high) * LOG2E)
            first += w
            second += w * w * yst[g, s, 1, at : at + 1, :]
        return high, first, second

    early, late = rows_of(range(GROUPS - 1)), rows_of([GROUPS - 1])
    for g in range(GROUPS - 1):
        got_stats(g)
    zero = jnp.zeros((NZ, LANE), jnp.float32)
    for j in range(NJ):
        held[j, 0], held[j, 1], held[j, 2] = merged(j, early, zero + BIG, zero, zero)
    got_stats(GROUPS - 1)
    for j in range(NJ):
        top, first, second = merged(j, late, held[j, 0], held[j, 1], held[j, 2])
        zsend[pl.ds(j, NZ, stride=8), :] = top + jnp.log(first)
        zsend[pl.ds(NJ + j, NZ, stride=8), :] = second / (first * first)

    heard(2)
    for zi, peer in zip(z_index, z_peers):
        remote(csend.at[zi], crecv.at[z], c_send, c_recv, peer)

    def block(index):
        return pl.ds(pl.multiple_of(index * 8, 8), 8)

    for zi, peer in zip(z_index, z_peers):
        remote(zsend.at[block(zi)], zrecv.at[block(z)], z_send, z_recv, peer)
    zrecv[block(z), :] = zsend[block(z), :]

    arrived(crecv.at[pl.ds(0, NZ - 1)], c_send, c_recv)
    total = crecv[0]
    for k in range(1, NZ):
        total += crecv[k]
    copies[2].wait()
    arrived(zrecv.at[pl.ds(0, 8 * (NZ - 1))], z_send, z_recv)
    top = zrecv[0:NJ, :]
    for k in range(1, NZ):
        top = jnp.maximum(top, zrecv[8 * k : 8 * k + NJ, :])
    first = jnp.zeros((NJ, LANE), jnp.float32)
    second = jnp.zeros((NJ, LANE), jnp.float32)
    for k in range(NZ):
        w = jnp.exp2((zrecv[8 * k : 8 * k + NJ, :] - top) * LOG2E)
        first += w
        second += w * w * zrecv[8 * k + NJ : 8 * k + 8, :]
    evidence = (top + jnp.log(first)) + offset_buf[...] - jnp.log(total)
    lbuf[z] = evidence
    for peer in z_peers:
        remote(lbuf.at[z], lbuf.at[z], l_send, l_recv, peer)
    evidence_out[...] = evidence
    ess_out[...] = first * first / (second * total)

    arrived(lbuf.at[pl.ds(0, NZ - 1)], l_send, l_recv)
    partial = lbuf[0]
    for k in range(1, NZ):
        partial += lbuf[k]
    vbuf[gi * NY + y] = partial
    for peer in v_peers:
        remote(vbuf.at[gi * NY + y], vbuf.at[gi * NY + y], v_send, v_recv, peer)
    arrived(vbuf.at[pl.ds(0, NG * NY - 1)], v_send, v_recv)

    def loglik(index):
        value = vbuf[index * NY]
        for k in range(1, NY):
            value += vbuf[index * NY + k]
        return value * (1.0 / EVENTS)

    lines = [loglik(k) for k in range(NG)]
    best = lines[0]
    for line in lines[1:]:
        best = jnp.maximum(best, line)
    best = jnp.max(best)
    mass = jnp.zeros((NJ, LANE), jnp.float32)
    for line in lines:
        mass += jnp.exp2((line - best) * LOG2E)
    mass = jnp.sum(mass)
    norm = best + jnp.log(jnp.full((NJ, LANE), mass))
    posterior_out[...] = loglik(gi) - norm

    for copy in sends:
        copy.wait_send()


def finish(evidence, ess, posterior, evidence_out, ess_out, posterior_out, sem):
    pairs = ((evidence, evidence_out), (ess, ess_out), (posterior, posterior_out))
    copies = [pltpu.make_async_copy(a, b, sem.at[k]) for k, (a, b) in enumerate(pairs)]
    for copy in copies:
        copy.start()
    for copy in copies:
        copy.wait()


def body(summary, weight, offset, prior, event, live):
    rows, bins = summary.shape
    cols = weight.shape[1]
    dma, vmem = pltpu.SemaphoreType.DMA, pltpu.VMEM
    f32 = jnp.float32
    small = jax.ShapeDtypeStruct((NJ, LANE), f32)
    kept = vmem((NJ, LANE), f32)
    hbm = pl.BlockSpec(memory_space=pltpu.HBM)
    smem = pl.BlockSpec(memory_space=pltpu.SMEM)
    outs = pl.pallas_call(
        kernel,
        name="reweight",
        out_shape=(kept, kept, kept),
        in_specs=[hbm, hbm, hbm, hbm, smem, smem],
        out_specs=(pl.BlockSpec(memory_space=pltpu.VMEM),) * 3,
        scratch_shapes=[
            vmem((rows, bins), jnp.bfloat16),
            vmem((bins, cols), jnp.bfloat16),
            vmem((2, rows // GROUPS, cols), f32),
            vmem((TILES, LANE), f32),
            vmem((NJ, LANE), f32),
            vmem((NY, 2, TILES, LANE), f32),
            vmem((GROUPS, NY, 2, PER * NJ, LANE), f32),
            vmem((NJ, 3, NZ, LANE), f32),
            vmem((NZ * 8, LANE), f32),
            vmem((NZ * 8, LANE), f32),
            vmem((NZ, 1, LANE), f32),
            vmem((NZ, 1, LANE), f32),
            vmem((NZ, NJ, LANE), f32),
            vmem((NG * NY, NJ, LANE), f32),
            dma((3 + GROUPS,)),
            dma((GROUPS,)),
            dma((GROUPS,)),
            dma, dma, dma, dma, dma, dma, dma, dma, dma, dma,
            pltpu.SemaphoreType.REGULAR((len(RELAY),)),
        ],
        compiler_params=pltpu.CompilerParams(
            collective_id=0, has_side_effects=True, vmem_limit_bytes=32 * 1024 * 1024
        ),
        cost_estimate=pl.CostEstimate(
            flops=2 * rows * bins * cols, bytes_accessed=2 * rows * bins, transcendentals=rows * cols
        ),
    )(*(
        pltpu.with_memory_space_constraint(a, pltpu.HBM)
        for a in (summary, weight, prior.reshape(TILES, LANE), offset.reshape(NJ, LANE), event, live)
    ))
    vm, any_space = pl.BlockSpec(memory_space=pltpu.VMEM), pl.BlockSpec(memory_space=pltpu.HBM)
    evidence, ess, posterior = pl.pallas_call(
        finish,
        name="finish",
        out_shape=(small, small, small),
        in_specs=[vm, vm, vm],
        out_specs=(any_space,) * 3,
        scratch_shapes=[dma((3,))],
        compiler_params=pltpu.CompilerParams(vmem_limit_bytes=1024 * 1024),
    )(*outs)
    return evidence.reshape(1, cols), ess.reshape(1, cols), posterior.reshape(cols)


def solution(mesh):
    in_specs = (P("samp", None), P(None, "grid"), P("grid"), P("samp"), P("samp"), P("samp"))
    out_specs = (P("samp", "grid"), P("samp", "grid"), P("grid"))
    return jax.shard_map(body, mesh=mesh, in_specs=in_specs, out_specs=out_specs, check_vma=False)
```

```python
import jax
import jax.numpy as jnp
from jax import lax
from jax.experimental import pallas as pl
from jax.experimental.pallas import tpu as pltpu
from jax.sharding import PartitionSpec as P

EVENTS = 64
NX, NC, NY, NZ = 4, 2, 4, 16
NG = NX * NC
TILE = 128
LANE = 128
NJ = 4
TILES = 16
OWN = EVENTS // NZ
SIZES = (256, 512, 512, 512, 256)
AHEAD = 2
HOP = 4
BIG = -1e30
LOG2E = 1.4426950408889634
MESH = pl.DeviceIdType.MESH


def kernel(
    summary, weight, prior, offset, event_in, live_in,
    evidence_out, ess_out, posterior_out,
    x_buf, w_buf, scores, prior_buf, offset_buf, event, live,
    yid, ysend, yrecv, held, zsend, zrecv, crecv, lbuf, osend, orecv, vbuf,
    in_sem, x_sem, id_send, id_recv, y_send, y_recv, c_send, c_recv, z_send, z_recv,
    l_send, l_recv, o_send, o_recv, v_send, v_recv, known,
):
    gi, si = lax.axis_index("grid"), lax.axis_index("samp")
    x, c = gi // NC, lax.rem(gi, NC)
    z, y = si // NY, lax.rem(si, NY)

    starts = [sum(SIZES[:g]) for g in range(len(SIZES))]
    x_copies = []
    for g, (at, size) in enumerate(zip(starts, SIZES)):
        part = pl.ds(at, size)
        x_copies.append(pltpu.make_async_copy(summary.at[part], x_buf.at[part], x_sem.at[g]))
    pairs = (
        (weight, w_buf), (prior, prior_buf), (event_in, event), (live_in, live), (offset, offset_buf)
    )
    w_copy, *small_copies = [
        pltpu.make_async_copy(a, b, in_sem.at[k]) for k, (a, b) in enumerate(pairs)
    ]
    w_copy.start()
    for copy in x_copies[:AHEAD]:
        copy.start()
    for copy in small_copies:
        copy.start()

    y_index = [lax.rem(y + d, NY) for d in range(1, NY)]
    y_peers = [(gi, z * NY + k) for k in y_index]
    z_index = [lax.rem(z + d, NZ) for d in range(1, NZ)]
    z_peers = [(gi, k * NY + y) for k in z_index]
    grid_peers, v_peers = [], []
    for dx in range(NX):
        for dc in range(NC):
            grid = lax.rem(x + dx, NX) * NC + lax.rem(c + dc, NC)
            if dx or dc:
                grid_peers.append((grid, si))
            for dy in range(NY):
                if dx or dc or dy:
                    v_peers.append((grid, z * NY + lax.rem(y + dy, NY)))

    near = y_peers + grid_peers + [z_peers[d - 1] for k in range(1, HOP + 1) for d in (k, NZ - k)]
    barrier = pltpu.get_barrier_semaphore()
    for peer in near:
        pl.semaphore_signal(barrier, inc=1, device_id=peer, device_id_type=MESH)

    lane = lax.broadcasted_iota(jnp.int32, (1, LANE), 1)

    def dot(g):
        x_copies[g].wait()
        if g + AHEAD < len(SIZES):
            x_copies[g + AHEAD].start()
        scores[g % 2, : SIZES[g], :] = jnp.dot(
            x_buf[starts[g] : starts[g] + SIZES[g], :], w_buf[...],
            preferred_element_type=jnp.float32,
        )

    def stats(g):
        for i in range(SIZES[g] // TILE):
            t = starts[g] // TILE + i
            add = jnp.where(lane < live[t], -prior_buf[t : t + 1, :], BIG)
            add = jnp.transpose(jnp.broadcast_to(add, (LANE, LANE)))
            for j in range(NJ):
                v = scores[g % 2, i * TILE : (i + 1) * TILE, j * LANE : (j + 1) * LANE] + add
                top = jnp.max(v, axis=0, keepdims=True)
                p = jnp.exp2((v - top) * LOG2E)
                first = jnp.sum(p, axis=0, keepdims=True)
                second = jnp.sum(p * p, axis=0, keepdims=True)
                ysend[j, t, 0:1, :] = top + jnp.log(first)
                ysend[j, t, 1:2, :] = second / (first * first)

    sends = []

    def remote(src, dst, send_sem, recv_sem, peer):
        copy = pltpu.make_async_remote_copy(
            src_ref=src, dst_ref=dst, send_sem=send_sem, recv_sem=recv_sem,
            device_id=peer, device_id_type=MESH,
        )
        copy.start()

    def arrived(ref, send_sem, recv_sem):
        copy = pltpu.make_async_remote_copy(
            src_ref=ref, dst_ref=ref, send_sem=send_sem, recv_sem=recv_sem,
            device_id=y_peers[0], device_id_type=MESH,
        )
        copy.wait_recv()
        sends.append(copy)

    split = starts[-1] // TILE
    batches = (pl.ds(0, split), pl.ds(split, TILES - split))

    def send_stats(b):
        for k, peer in zip(y_index, y_peers):
            remote(
                ysend.at[k, batches[b]], yrecv.at[y, batches[b]], y_send.at[b], y_recv.at[b], peer
            )

    def got_stats(b):
        yrecv[y, batches[b]] = ysend[y, batches[b]]
        size = TILES - split if b else split
        whole = yrecv.at[pl.ds(0, NY - 1), pl.ds(0, size)]
        arrived(whole, y_send.at[b], y_recv.at[b])

    w_copy.wait()
    dot(0)
    for copy in small_copies:
        copy.wait()
    count = jnp.zeros((1, LANE), jnp.float32)
    for t in range(TILES):
        yid[y, t] = jnp.full((1, LANE), event[t].astype(jnp.float32))
        count += jnp.where(lane == event[t], live[t].astype(jnp.float32), 0.0)
    yid[y, TILES] = count
    for g in range(1, len(SIZES)):
        dot(g)
        stats(g - 1)
    pl.semaphore_wait(barrier, len(near))
    for peer in y_peers:
        remote(yid.at[y], yid.at[y], id_send, id_recv, peer)
    send_stats(0)
    for d in (HOP, NZ - HOP):
        pl.semaphore_signal(known, inc=1, device_id=z_peers[d - 1], device_id_type=MESH)
    stats(len(SIZES) - 1)
    send_stats(1)

    arrived(yid.at[pl.ds(0, NY - 1)], id_send, id_recv)
    count = yid[0, TILES]
    for s in range(1, NY):
        count += yid[s, TILES]
    crecv[z] = count
    index = lax.broadcasted_iota(jnp.int32, (EVENTS, LANE), 0).astype(jnp.float32)

    def chosen(s, t):
        member = jnp.broadcast_to(yid[s, t], (EVENTS, LANE)) == index
        return jnp.where(member, yrecv[s, t, 0:1, :], BIG)

    def merged(order, top, first, second):
        high = top
        for entry in order:
            high = jnp.maximum(high, chosen(*entry))
        keep = jnp.exp2((top - high) * LOG2E)
        first, second = first * keep, second * (keep * keep)
        for s, t in order:
            w = jnp.exp2((chosen(s, t) - high) * LOG2E)
            first += w
            second += w * w * yrecv[s, t, 1:2, :]
        return high, first, second

    zero = jnp.zeros((EVENTS, LANE), jnp.float32)
    got_stats(0)
    order = [(s, t) for t in range(split) for s in range(NY)]
    held[0], held[1], held[2] = merged(order, zero + BIG, zero, zero)
    got_stats(1)
    order = [(s, t) for t in range(split, TILES) for s in range(NY)]
    top, first, second = merged(order, held[0], held[1], held[2])
    lse, ratio = top + jnp.log(first), second / (first * first)
    for k in range(NZ):
        zsend[k, 0] = lse[k * OWN : (k + 1) * OWN, :]
        zsend[k, 1] = ratio[k * OWN : (k + 1) * OWN, :]

    pl.semaphore_wait(known, 2)
    for peer in z_peers:
        remote(crecv.at[z], crecv.at[z], c_send, c_recv, peer)
    for k, peer in zip(z_index, z_peers):
        remote(zsend.at[k], zrecv.at[z], z_send, z_recv, peer)
    zrecv[z] = zsend[z]

    arrived(crecv.at[pl.ds(0, NZ - 1)], c_send, c_recv)
    count = crecv[0]
    for k in range(1, NZ):
        count += crecv[k]
    row = lax.broadcasted_iota(jnp.int32, (OWN, LANE), 0)
    col = lax.broadcasted_iota(jnp.int32, (OWN, LANE), 1)
    count = jnp.where(col == row + z * OWN, jnp.broadcast_to(count, (OWN, LANE)), 0.0)
    count = jnp.broadcast_to(jnp.sum(count, axis=1, keepdims=True), (OWN, LANE))
    shift = offset_buf[pl.ds(y, 1), :] - jnp.log(count)
    arrived(zrecv.at[pl.ds(0, NZ - 1)], z_send, z_recv)
    top = zrecv[0, 0]
    for k in range(1, NZ):
        top = jnp.maximum(top, zrecv[k, 0])
    first = jnp.zeros((OWN, LANE), jnp.float32)
    second = jnp.zeros((OWN, LANE), jnp.float32)
    for k in range(NZ):
        w = jnp.exp2((zrecv[k, 0] - top) * LOG2E)
        first += w
        second += w * w * zrecv[k, 1]
    evidence = top + jnp.log(first) + shift
    lbuf[z] = jnp.sum(evidence, axis=0, keepdims=True)
    for peer in z_peers:
        remote(lbuf.at[z], lbuf.at[z], l_send, l_recv, peer)
    ess = first * first / (second * count)
    for i in range(NY):
        osend[i, 0:1, :] = evidence[i : i + 1, :]
        osend[i, 1:2, :] = ess[i : i + 1, :]
    for k, peer in zip(y_index, y_peers):
        remote(osend.at[k], orecv.at[y], o_send, o_recv, peer)
    orecv[y] = osend[y]

    arrived(lbuf.at[pl.ds(0, NZ - 1)], l_send, l_recv)
    loglik = lbuf[0]
    for k in range(1, NZ):
        loglik += lbuf[k]
    vbuf[gi * NJ + y] = loglik * (1.0 / EVENTS)
    for peer in v_peers:
        remote(vbuf.at[gi * NJ + y], vbuf.at[gi * NJ + y], v_send, v_recv, peer)
    arrived(orecv.at[pl.ds(0, NY - 1)], o_send, o_recv)
    for j in range(NJ):
        evidence_out[j : j + 1, :] = orecv[j, 0:1, :]
        ess_out[j : j + 1, :] = orecv[j, 1:2, :]
    arrived(vbuf.at[pl.ds(0, NG * NJ - 1)], v_send, v_recv)
    best = vbuf[0]
    for k in range(1, NG * NJ):
        best = jnp.maximum(best, vbuf[k])
    best = jnp.max(best)
    mass = jnp.zeros((1, LANE), jnp.float32)
    for k in range(NG * NJ):
        mass += jnp.exp2((vbuf[k] - best) * LOG2E)
    norm = best + jnp.log(jnp.full((1, LANE), jnp.sum(mass)))
    for j in range(NJ):
        posterior_out[j : j + 1, :] = vbuf[gi * NJ + j] - norm

    for copy in sends:
        copy.wait_send()


def finish(evidence, ess, posterior, evidence_out, ess_out, posterior_out, sem):
    pairs = ((evidence, evidence_out), (ess, ess_out), (posterior, posterior_out))
    copies = [pltpu.make_async_copy(a, b, sem.at[k]) for k, (a, b) in enumerate(pairs)]
    for copy in copies:
        copy.start()
    for copy in copies:
        copy.wait()


def body(summary, weight, offset, prior, event, live):
    rows, bins = summary.shape
    cols = weight.shape[1]
    dma, vmem, smem = pltpu.SemaphoreType.DMA, pltpu.VMEM, pltpu.SMEM
    f32 = jnp.float32
    hbm = pl.BlockSpec(memory_space=pltpu.HBM)
    local = pl.BlockSpec(memory_space=pltpu.VMEM)
    kept = vmem((NJ, LANE), f32)
    outs = pl.pallas_call(
        kernel,
        name="reweight",
        out_shape=(kept, kept, kept),
        in_specs=[hbm] * 6,
        out_specs=(local,) * 3,
        scratch_shapes=[
            vmem((rows, bins), jnp.bfloat16),
            vmem((bins, cols), jnp.bfloat16),
            vmem((2, max(SIZES), cols), f32),
            vmem((TILES, LANE), f32),
            vmem((NJ, LANE), f32),
            smem((TILES,), jnp.int32),
            smem((TILES,), jnp.int32),
            vmem((NY, TILES + 1, 1, LANE), f32),
            vmem((NJ, TILES, 2, LANE), f32),
            vmem((NY, TILES, 2, LANE), f32),
            vmem((3, EVENTS, LANE), f32),
            vmem((NZ, 2, OWN, LANE), f32),
            vmem((NZ, 2, OWN, LANE), f32),
            vmem((NZ, 1, LANE), f32),
            vmem((NZ, 1, LANE), f32),
            vmem((NY, 2, LANE), f32),
            vmem((NY, 2, LANE), f32),
            vmem((NG * NJ, 1, LANE), f32),
            dma((5,)),
            dma((len(SIZES),)),
            dma, dma,
            dma((2,)),
            dma((2,)),
            dma, dma, dma, dma, dma, dma, dma, dma, dma, dma,
            pltpu.SemaphoreType.REGULAR,
        ],
        compiler_params=pltpu.CompilerParams(
            collective_id=0, has_side_effects=True, vmem_limit_bytes=32 * 1024 * 1024
        ),
        cost_estimate=pl.CostEstimate(
            flops=2 * rows * bins * cols, bytes_accessed=2 * rows * bins, transcendentals=rows * cols
        ),
    )(*(
        pltpu.with_memory_space_constraint(a, pltpu.HBM)
        for a in (summary, weight, prior.reshape(TILES, LANE), offset.reshape(NJ, LANE), event, live)
    ))
    small = jax.ShapeDtypeStruct((NJ, LANE), f32)
    evidence, ess, posterior = pl.pallas_call(
        finish,
        name="finish",
        out_shape=(small, small, small),
        in_specs=[local] * 3,
        out_specs=(hbm,) * 3,
        scratch_shapes=[dma((3,))],
        compiler_params=pltpu.CompilerParams(vmem_limit_bytes=1024 * 1024),
    )(*outs)
    return evidence.reshape(1, cols), ess.reshape(1, cols), posterior.reshape(cols)


def solution(mesh):
    in_specs = (P("samp", None), P(None, "grid"), P("grid"), P("samp"), P("samp"), P("samp"))
    out_specs = (P("samp", "grid"), P("samp", "grid"), P("grid"))
    return jax.shard_map(body, mesh=mesh, in_specs=in_specs, out_specs=out_specs, check_vma=False)
```

```python
import jax
import jax.numpy as jnp
from jax import lax
from jax.experimental import pallas as pl
from jax.experimental.pallas import tpu as pltpu
from jax.sharding import PartitionSpec as P

EVENTS = 64
NX, NC, NY, NZ = 4, 2, 4, 16
NG = NX * NC
TILE = 128
LANE = 128
NJ = 4
TILES = 16
OWN = EVENTS // NZ
SIZES = (256, 512, 512, 512, 256)
WAITS = 3
ROOT = 0
HOP = 4
BIG = -1e30
LOG2E = 1.4426950408889634
MESH = pl.DeviceIdType.MESH


def kernel(
    summary, weight, prior, offset, event_in, live_in,
    evidence_out, ess_out, posterior_out,
    x_buf, w_buf, scores, prior_buf, offset_buf, event, live,
    yid, ysend, yrecv, held, lse, lse_all, zsend, zrecv, crecv, osend, orecv, vbuf, pbuf,
    in_sem, x_sem, id_send, id_recv, y_send, y_recv, c_send, c_recv, z_send, z_recv,
    l_send, l_recv, o_send, o_recv, v_send, v_recv, p_send, p_recv, known,
):
    gi, si = lax.axis_index("grid"), lax.axis_index("samp")
    x, c = gi // NC, lax.rem(gi, NC)
    z, y = si // NY, lax.rem(si, NY)

    starts = [sum(SIZES[:g]) for g in range(len(SIZES))]
    x_copies = []
    for g, (at, size) in enumerate(zip(starts, SIZES)):
        part = pl.ds(at, size)
        x_copies.append(pltpu.make_async_copy(summary.at[part], x_buf.at[part], x_sem.at[g]))
    pairs = (
        (weight, w_buf), (prior, prior_buf), (event_in, event), (live_in, live), (offset, offset_buf)
    )
    w_copy, *small_copies = [
        pltpu.make_async_copy(a, b, in_sem.at[k]) for k, (a, b) in enumerate(pairs)
    ]
    for copy in (*small_copies, w_copy, *x_copies):
        copy.start()

    y_index = [lax.rem(y + d, NY) for d in range(1, NY)]
    y_peers = [(gi, z * NY + k) for k in y_index]
    z_index = [lax.rem(z + d, NZ) for d in range(1, NZ)]
    z_peers = [(gi, k * NY + y) for k in z_index]
    grid_peers, v_peers = [], []
    for dx in range(NX):
        for dc in range(NC):
            grid = lax.rem(x + dx, NX) * NC + lax.rem(c + dc, NC)
            if dx or dc:
                grid_peers.append((grid, si))
            for dy in range(NY):
                if dx or dc or dy:
                    v_peers.append((grid, z * NY + lax.rem(y + dy, NY)))

    near = y_peers + grid_peers + [z_peers[d - 1] for k in range(1, HOP + 1) for d in (k, NZ - k)]
    barrier = pltpu.get_barrier_semaphore()
    for peer in near:
        pl.semaphore_signal(barrier, inc=1, device_id=peer, device_id_type=MESH)

    lane = lax.broadcasted_iota(jnp.int32, (1, LANE), 1)

    def dot(g):
        if g < WAITS:
            for copy in x_copies[g:] if g == WAITS - 1 else x_copies[g : g + 1]:
                copy.wait()
        scores[g % 2, : SIZES[g], :] = jnp.dot(
            x_buf[starts[g] : starts[g] + SIZES[g], :], w_buf[...],
            preferred_element_type=jnp.float32,
        )

    def stats(g):
        for i in range(SIZES[g] // TILE):
            t = starts[g] // TILE + i
            add = jnp.where(lane < live[t], -prior_buf[t : t + 1, :], BIG)
            add = jnp.transpose(jnp.broadcast_to(add, (LANE, LANE)))
            for j in range(NJ):
                v = scores[g % 2, i * TILE : (i + 1) * TILE, j * LANE : (j + 1) * LANE] + add
                top = jnp.max(v, axis=0, keepdims=True)
                p = jnp.exp2((v - top) * LOG2E)
                first = jnp.sum(p, axis=0, keepdims=True)
                second = jnp.sum(p * p, axis=0, keepdims=True)
                ysend[j, t, 0:1, :] = top + jnp.log(first)
                ysend[j, t, 1:2, :] = second / (first * first)

    def remote(src, dst, send_sem, recv_sem, peer):
        copy = pltpu.make_async_remote_copy(
            src_ref=src, dst_ref=dst, send_sem=send_sem, recv_sem=recv_sem,
            device_id=peer, device_id_type=MESH,
        )
        copy.start()

    def moved(ref, send_sem, recv_sem):
        return pltpu.make_async_remote_copy(
            src_ref=ref, dst_ref=ref, send_sem=send_sem, recv_sem=recv_sem,
            device_id=y_peers[0], device_id_type=MESH,
        )

    id_moved = moved(yid.at[pl.ds(0, NY - 1)], id_send, id_recv)
    c_moved = moved(crecv.at[pl.ds(0, NZ - 1)], c_send, c_recv)
    z_moved = moved(zrecv.at[pl.ds(0, NZ - 1)], z_send, z_recv)
    o_moved = moved(orecv.at[pl.ds(0, NY - 1)], o_send, o_recv)

    split = starts[-1] // TILE
    batches = (pl.ds(0, split), pl.ds(split, TILES - split))

    def send_stats(b):
        for k, peer in zip(y_index, y_peers):
            remote(
                ysend.at[k, batches[b]], yrecv.at[y, batches[b]], y_send.at[b], y_recv.at[b], peer
            )

    def stats_moved(b):
        size = TILES - split if b else split
        return moved(yrecv.at[pl.ds(0, NY - 1), pl.ds(0, size)], y_send.at[b], y_recv.at[b])

    def got_stats(b):
        yrecv[y, batches[b]] = ysend[y, batches[b]]
        stats_moved(b).wait_recv()

    for copy in small_copies:
        copy.wait()
    count = jnp.zeros((1, LANE), jnp.float32)
    for t in range(TILES):
        yid[y, t] = jnp.full((1, LANE), event[t].astype(jnp.float32))
        count += jnp.where(lane == event[t], live[t].astype(jnp.float32), 0.0)
    yid[y, TILES] = count
    w_copy.wait()
    dot(0)
    for g in range(1, len(SIZES)):
        dot(g)
        stats(g - 1)
    pl.semaphore_wait(barrier, len(near))
    for peer in y_peers:
        remote(yid.at[y], yid.at[y], id_send, id_recv, peer)
    send_stats(0)
    for d in (HOP, NZ - HOP):
        pl.semaphore_signal(known, inc=1, device_id=z_peers[d - 1], device_id_type=MESH)
    stats(len(SIZES) - 1)
    send_stats(1)

    id_moved.wait_recv()
    count = yid[0, TILES]
    for s in range(1, NY):
        count += yid[s, TILES]
    crecv[z] = count
    index = lax.broadcasted_iota(jnp.int32, (EVENTS, LANE), 0).astype(jnp.float32)

    def chosen(s, t):
        member = jnp.broadcast_to(yid[s, t], (EVENTS, LANE)) == index
        return jnp.where(member, yrecv[s, t, 0:1, :], BIG)

    def merged(order, top, first, second):
        high = top
        for entry in order:
            high = jnp.maximum(high, chosen(*entry))
        keep = jnp.exp2((top - high) * LOG2E)
        first, second = first * keep, second * (keep * keep)
        for s, t in order:
            w = jnp.exp2((chosen(s, t) - high) * LOG2E)
            first += w
            second += w * w * yrecv[s, t, 1:2, :]
        return high, first, second

    zero = jnp.zeros((EVENTS, LANE), jnp.float32)
    got_stats(0)
    order = [(s, t) for t in range(split) for s in range(NY)]
    held[0], held[1], held[2] = merged(order, zero + BIG, zero, zero)
    pl.semaphore_wait(known, 2)
    for peer in z_peers:
        remote(crecv.at[z], crecv.at[z], c_send, c_recv, peer)
    got_stats(1)
    order = [(s, t) for t in range(split, TILES) for s in range(NY)]
    top, first, second = merged(order, held[0], held[1], held[2])
    lse[...] = top + jnp.log(first)

    @pl.when(z != ROOT)
    def _():
        remote(lse, lse_all.at[z], l_send, l_recv, (gi, ROOT * NY + y))

    ratio = second / (first * first)
    for k in range(NZ):
        zsend[k, 0] = lse[k * OWN : (k + 1) * OWN, :]
        zsend[k, 1] = ratio[k * OWN : (k + 1) * OWN, :]
    for k, peer in zip(z_index, z_peers):
        remote(zsend.at[k], zrecv.at[z], z_send, z_recv, peer)
    zrecv[z] = zsend[z]

    c_moved.wait_recv()
    count = crecv[0]
    for k in range(1, NZ):
        count += crecv[k]
    shift = offset_buf[pl.ds(y, 1), :]
    v_moved = moved(vbuf.at[pl.ds(0, NG * NJ - 1)], v_send, v_recv)

    @pl.when(z == ROOT)
    def _():
        logs = jnp.sum(jnp.where(lane < EVENTS, jnp.log(jnp.maximum(count, 1.0)), 0.0))
        lse_all[ROOT] = lse[...]
        moved(lse_all.at[pl.ds(0, NZ - 1)], l_send, l_recv).wait_recv()
        top = lse_all[0]
        for k in range(1, NZ):
            top = jnp.maximum(top, lse_all[k])
        first = jnp.zeros((EVENTS, LANE), jnp.float32)
        for k in range(NZ):
            first += jnp.exp2((lse_all[k] - top) * LOG2E)
        line = jnp.sum(top + jnp.log(first), axis=0, keepdims=True)
        vbuf[gi * NJ + y] = (line - logs) * (1.0 / EVENTS) + shift
        for peer in v_peers:
            remote(vbuf.at[gi * NJ + y], vbuf.at[gi * NJ + y], v_send, v_recv, peer)

    row = lax.broadcasted_iota(jnp.int32, (OWN, LANE), 0)
    col = lax.broadcasted_iota(jnp.int32, (OWN, LANE), 1)
    count = jnp.where(col == row + z * OWN, jnp.broadcast_to(count, (OWN, LANE)), 0.0)
    count = jnp.broadcast_to(jnp.sum(count, axis=1, keepdims=True), (OWN, LANE))
    shift = shift - jnp.log(count)
    z_moved.wait_recv()
    top = zrecv[0, 0]
    for k in range(1, NZ):
        top = jnp.maximum(top, zrecv[k, 0])
    first = jnp.zeros((OWN, LANE), jnp.float32)
    second = jnp.zeros((OWN, LANE), jnp.float32)
    for k in range(NZ):
        w = jnp.exp2((zrecv[k, 0] - top) * LOG2E)
        first += w
        second += w * w * zrecv[k, 1]
    evidence = top + jnp.log(first) + shift
    ess = first * first / (second * count)
    for i in range(NY):
        osend[i, 0:1, :] = evidence[i : i + 1, :]
        osend[i, 1:2, :] = ess[i : i + 1, :]
    for k, peer in zip(y_index, y_peers):
        remote(osend.at[k], orecv.at[y], o_send, o_recv, peer)
    orecv[y] = osend[y]

    @pl.when(z == ROOT)
    def _():
        v_moved.wait_recv()
        best = vbuf[0]
        for k in range(1, NG * NJ):
            best = jnp.maximum(best, vbuf[k])
        best = jnp.max(best)
        mass = jnp.zeros((1, LANE), jnp.float32)
        for k in range(NG * NJ):
            mass += jnp.exp2((vbuf[k] - best) * LOG2E)
        norm = best + jnp.log(jnp.full((1, LANE), jnp.sum(mass)))
        for j in range(NJ):
            pbuf[j : j + 1, :] = vbuf[gi * NJ + j] - norm
        for peer in z_peers:
            remote(pbuf, pbuf, p_send, p_recv, peer)

    o_moved.wait_recv()
    for j in range(NJ):
        evidence_out[j : j + 1, :] = orecv[j, 0:1, :]
        ess_out[j : j + 1, :] = orecv[j, 1:2, :]

    for copy in (id_moved, c_moved, z_moved, o_moved, stats_moved(0), stats_moved(1)):
        copy.wait_send()

    @pl.when(z != ROOT)
    def _():
        moved(lse, l_send, l_recv).wait_send()
        moved(pbuf, p_send, p_recv).wait_recv()

    @pl.when(z == ROOT)
    def _():
        v_moved.wait_send()
        for _ in range(NZ - 1):
            moved(pbuf, p_send, p_recv).wait_send()

    posterior_out[...] = pbuf[...]


def finish(evidence, ess, posterior, evidence_out, ess_out, posterior_out, sem):
    pairs = ((evidence, evidence_out), (ess, ess_out), (posterior, posterior_out))
    copies = [pltpu.make_async_copy(a, b, sem.at[k]) for k, (a, b) in enumerate(pairs)]
    for copy in copies:
        copy.start()
    for copy in copies:
        copy.wait()


def body(summary, weight, offset, prior, event, live):
    rows, bins = summary.shape
    cols = weight.shape[1]
    dma, vmem, smem = pltpu.SemaphoreType.DMA, pltpu.VMEM, pltpu.SMEM
    f32 = jnp.float32
    hbm = pl.BlockSpec(memory_space=pltpu.HBM)
    local = pl.BlockSpec(memory_space=pltpu.VMEM)
    kept = vmem((NJ, LANE), f32)
    outs = pl.pallas_call(
        kernel,
        name="reweight",
        out_shape=(kept, kept, kept),
        in_specs=[hbm] * 6,
        out_specs=(local,) * 3,
        scratch_shapes=[
            vmem((rows, bins), jnp.bfloat16),
            vmem((bins, cols), jnp.bfloat16),
            vmem((2, max(SIZES), cols), f32),
            vmem((TILES, LANE), f32),
            vmem((NJ, LANE), f32),
            smem((TILES,), jnp.int32),
            smem((TILES,), jnp.int32),
            vmem((NY, TILES + 1, 1, LANE), f32),
            vmem((NJ, TILES, 2, LANE), f32),
            vmem((NY, TILES, 2, LANE), f32),
            vmem((3, EVENTS, LANE), f32),
            vmem((EVENTS, LANE), f32),
            vmem((NZ, EVENTS, LANE), f32),
            vmem((NZ, 2, OWN, LANE), f32),
            vmem((NZ, 2, OWN, LANE), f32),
            vmem((NZ, 1, LANE), f32),
            vmem((NY, 2, LANE), f32),
            vmem((NY, 2, LANE), f32),
            vmem((NG * NJ, 1, LANE), f32),
            vmem((NJ, LANE), f32),
            dma((5,)),
            dma((len(SIZES),)),
            dma, dma,
            dma((2,)),
            dma((2,)),
            dma, dma, dma, dma, dma, dma, dma, dma, dma, dma, dma, dma,
            pltpu.SemaphoreType.REGULAR,
        ],
        compiler_params=pltpu.CompilerParams(
            collective_id=0, has_side_effects=True, vmem_limit_bytes=32 * 1024 * 1024
        ),
        cost_estimate=pl.CostEstimate(
            flops=2 * rows * bins * cols, bytes_accessed=2 * rows * bins, transcendentals=rows * cols
        ),
    )(*(
        pltpu.with_memory_space_constraint(a, pltpu.HBM)
        for a in (summary, weight, prior.reshape(TILES, LANE), offset.reshape(NJ, LANE), event, live)
    ))
    small = jax.ShapeDtypeStruct((NJ, LANE), f32)
    evidence, ess, posterior = pl.pallas_call(
        finish,
        name="finish",
        out_shape=(small, small, small),
        in_specs=[local] * 3,
        out_specs=(hbm,) * 3,
        scratch_shapes=[dma((3,))],
        compiler_params=pltpu.CompilerParams(vmem_limit_bytes=1024 * 1024),
    )(*outs)
    return evidence.reshape(1, cols), ess.reshape(1, cols), posterior.reshape(cols)


def solution(mesh):
    in_specs = (P("samp", None), P(None, "grid"), P("grid"), P("samp"), P("samp"), P("samp"))
    out_specs = (P("samp", "grid"), P("samp", "grid"), P("grid"))
    return jax.shard_map(body, mesh=mesh, in_specs=in_specs, out_specs=out_specs, check_vma=False)
```

```python
import jax
import jax.numpy as jnp
from jax import lax
from jax.experimental import pallas as pl
from jax.experimental.pallas import tpu as pltpu
from jax.sharding import PartitionSpec as P

EVENTS = 64
NX, NC, NY, NZ = 4, 2, 4, 16
NG = NX * NC
TILE = 128
LANE = 128
NJ = 4
TILES = 16
SIZES = (256, 512, 512, 512, 256)
WAITS = 3
ROOT = 0
HOP = 4
BIG = -1e30
LOG2E = 1.4426950408889634
MESH = pl.DeviceIdType.MESH


def kernel(
    summary, weight, prior, offset, event_in, live_in,
    evidence_out, ess_out, posterior_out,
    x_buf, w_buf, scores, prior_buf, offset_buf, event, live,
    yid, ysend, yrecv, held, lse, lse_all, zsend, zrecv, crecv, vbuf, pbuf,
    in_sem, x_sem, id_send, id_recv, y_send, y_recv, c_send, c_recv, z_send, z_recv,
    l_send, l_recv, v_send, v_recv, p_send, p_recv, known,
):
    gi, si = lax.axis_index("grid"), lax.axis_index("samp")
    x, c = gi // NC, lax.rem(gi, NC)
    z, y = si // NY, lax.rem(si, NY)

    starts = [sum(SIZES[:g]) for g in range(len(SIZES))]
    x_copies = []
    for g, (at, size) in enumerate(zip(starts, SIZES)):
        part = pl.ds(at, size)
        x_copies.append(pltpu.make_async_copy(summary.at[part], x_buf.at[part], x_sem.at[g]))
    pairs = (
        (weight, w_buf), (prior, prior_buf), (event_in, event), (live_in, live), (offset, offset_buf)
    )
    w_copy, *small_copies = [
        pltpu.make_async_copy(a, b, in_sem.at[k]) for k, (a, b) in enumerate(pairs)
    ]
    for copy in (*small_copies, w_copy, *x_copies):
        copy.start()

    y_index = [lax.rem(y + d, NY) for d in range(1, NY)]
    y_peers = [(gi, z * NY + k) for k in y_index]
    z_index = [lax.rem(z + d, NZ) for d in range(1, NZ)]
    z_peers = [(gi, k * NY + y) for k in z_index]
    grid_peers, v_peers = [], []
    for dx in range(NX):
        for dc in range(NC):
            grid = lax.rem(x + dx, NX) * NC + lax.rem(c + dc, NC)
            if dx or dc:
                grid_peers.append((grid, si))
            for dy in range(NY):
                if dx or dc or dy:
                    v_peers.append((grid, z * NY + lax.rem(y + dy, NY)))

    near = y_peers + grid_peers + [z_peers[d - 1] for k in range(1, HOP + 1) for d in (k, NZ - k)]
    barrier = pltpu.get_barrier_semaphore()
    for peer in near:
        pl.semaphore_signal(barrier, inc=1, device_id=peer, device_id_type=MESH)

    lane = lax.broadcasted_iota(jnp.int32, (1, LANE), 1)

    def dot(g):
        if g < WAITS:
            for copy in x_copies[g:] if g == WAITS - 1 else x_copies[g : g + 1]:
                copy.wait()
        scores[g % 2, : SIZES[g], :] = jnp.dot(
            x_buf[starts[g] : starts[g] + SIZES[g], :], w_buf[...],
            preferred_element_type=jnp.float32,
        )

    def stats(g):
        for i in range(SIZES[g] // TILE):
            t = starts[g] // TILE + i
            add = jnp.where(lane < live[t], -prior_buf[t : t + 1, :], BIG)
            add = jnp.transpose(jnp.broadcast_to(add, (LANE, LANE)))
            for j in range(NJ):
                v = scores[g % 2, i * TILE : (i + 1) * TILE, j * LANE : (j + 1) * LANE] + add
                top = jnp.max(v, axis=0, keepdims=True)
                p = jnp.exp2((v - top) * LOG2E)
                first = jnp.sum(p, axis=0, keepdims=True)
                second = jnp.sum(p * p, axis=0, keepdims=True)
                ysend[j, t, 0:1, :] = top + jnp.log(first)
                ysend[j, t, 1:2, :] = second / (first * first)

    def remote(src, dst, send_sem, recv_sem, peer):
        copy = pltpu.make_async_remote_copy(
            src_ref=src, dst_ref=dst, send_sem=send_sem, recv_sem=recv_sem,
            device_id=peer, device_id_type=MESH,
        )
        copy.start()

    def moved(ref, send_sem, recv_sem):
        return pltpu.make_async_remote_copy(
            src_ref=ref, dst_ref=ref, send_sem=send_sem, recv_sem=recv_sem,
            device_id=y_peers[0], device_id_type=MESH,
        )

    id_moved = moved(yid.at[pl.ds(0, NY - 1)], id_send, id_recv)
    c_moved = moved(crecv.at[pl.ds(0, NZ - 1)], c_send, c_recv)
    z_moved = moved(zrecv.at[pl.ds(0, EVENTS - 1)], z_send, z_recv)

    split = starts[-1] // TILE
    batches = (pl.ds(0, split), pl.ds(split, TILES - split))

    def send_stats(b):
        for k, peer in zip(y_index, y_peers):
            remote(
                ysend.at[k, batches[b]], yrecv.at[y, batches[b]], y_send.at[b], y_recv.at[b], peer
            )

    def stats_moved(b):
        size = TILES - split if b else split
        return moved(yrecv.at[pl.ds(0, NY - 1), pl.ds(0, size)], y_send.at[b], y_recv.at[b])

    def got_stats(b):
        yrecv[y, batches[b]] = ysend[y, batches[b]]
        stats_moved(b).wait_recv()

    for copy in small_copies:
        copy.wait()
    count = jnp.zeros((1, LANE), jnp.float32)
    for t in range(TILES):
        yid[y, t] = jnp.full((1, LANE), event[t].astype(jnp.float32))
        count += jnp.where(lane == event[t], live[t].astype(jnp.float32), 0.0)
    yid[y, TILES] = count
    w_copy.wait()
    dot(0)
    for g in range(1, len(SIZES)):
        dot(g)
        stats(g - 1)
    pl.semaphore_wait(barrier, len(near))
    for peer in y_peers:
        remote(yid.at[y], yid.at[y], id_send, id_recv, peer)
    send_stats(0)
    for d in (HOP, NZ - HOP):
        pl.semaphore_signal(known.at[0], inc=1, device_id=z_peers[d - 1], device_id_type=MESH)
    stats(len(SIZES) - 1)
    send_stats(1)

    id_moved.wait_recv()
    count = yid[0, TILES]
    for s in range(1, NY):
        count += yid[s, TILES]
    crecv[z] = count
    index = lax.broadcasted_iota(jnp.int32, (EVENTS, LANE), 0).astype(jnp.float32)

    def chosen(s, t):
        member = jnp.broadcast_to(yid[s, t], (EVENTS, LANE)) == index
        return jnp.where(member, yrecv[s, t, 0:1, :], BIG)

    def merged(order, top, first, second):
        high = top
        for entry in order:
            high = jnp.maximum(high, chosen(*entry))
        keep = jnp.exp2((top - high) * LOG2E)
        first, second = first * keep, second * (keep * keep)
        for s, t in order:
            w = jnp.exp2((chosen(s, t) - high) * LOG2E)
            first += w
            second += w * w * yrecv[s, t, 1:2, :]
        return high, first, second

    zero = jnp.zeros((EVENTS, LANE), jnp.float32)
    got_stats(0)
    order = [(s, t) for t in range(split) for s in range(NY)]
    held[0], held[1], held[2] = merged(order, zero + BIG, zero, zero)
    pl.semaphore_wait(known.at[0], 2)
    for peer in y_peers:
        pl.semaphore_signal(known.at[1], inc=1, device_id=peer, device_id_type=MESH)
    for peer in z_peers:
        remote(crecv.at[z], crecv.at[z], c_send, c_recv, peer)
    got_stats(1)
    order = [(s, t) for t in range(split, TILES) for s in range(NY)]
    top, first, second = merged(order, held[0], held[1], held[2])
    lse[...] = top + jnp.log(first)

    @pl.when(z != ROOT)
    def _():
        remote(lse, lse_all.at[z], l_send, l_recv, (gi, ROOT * NY + y))

    ratio = second / (first * first)
    for k in range(EVENTS):
        zsend[k, 0:1, :] = lse[k : k + 1, :]
        zsend[k, 1:2, :] = ratio[k : k + 1, :]
    zrecv[si] = zsend[si]
    pl.semaphore_wait(known.at[1], NY - 1)
    c_moved.wait_recv()
    for dz in sorted(range(NZ), key=lambda d: abs(d - NZ // 2)):
        for dy in range(NY):
            if dz or dy:
                k = lax.rem(z + dz, NZ) * NY + lax.rem(y + dy, NY)
                remote(zsend.at[k], zrecv.at[si], z_send, z_recv, (gi, k))

    count = crecv[0]
    for k in range(1, NZ):
        count += crecv[k]
    v_moved = moved(vbuf.at[pl.ds(0, NG * NJ - 1)], v_send, v_recv)

    @pl.when(z == ROOT)
    def _():
        logs = jnp.sum(jnp.where(lane < EVENTS, jnp.log(jnp.maximum(count, 1.0)), 0.0))
        lse_all[ROOT] = lse[...]
        moved(lse_all.at[pl.ds(0, NZ - 1)], l_send, l_recv).wait_recv()
        top = lse_all[0]
        for k in range(1, NZ):
            top = jnp.maximum(top, lse_all[k])
        first = jnp.zeros((EVENTS, LANE), jnp.float32)
        for k in range(NZ):
            first += jnp.exp2((lse_all[k] - top) * LOG2E)
        line = jnp.sum(top + jnp.log(first), axis=0, keepdims=True)
        vbuf[gi * NJ + y] = (line - logs) * (1.0 / EVENTS) + offset_buf[pl.ds(y, 1), :]
        for peer in v_peers:
            remote(vbuf.at[gi * NJ + y], vbuf.at[gi * NJ + y], v_send, v_recv, peer)

    count = jnp.full((1, LANE), jnp.sum(jnp.where(lane == si, count, 0.0)))
    z_moved.wait_recv()
    for j in range(NJ):
        top = zrecv[j, 0:1, :]
        for k in range(1, NZ):
            top = jnp.maximum(top, zrecv[k * NY + j, 0:1, :])
        first = jnp.zeros((1, LANE), jnp.float32)
        second = jnp.zeros((1, LANE), jnp.float32)
        for k in range(NZ):
            w = jnp.exp2((zrecv[k * NY + j, 0:1, :] - top) * LOG2E)
            first += w
            second += w * w * zrecv[k * NY + j, 1:2, :]
        shift = offset_buf[j : j + 1, :] - jnp.log(count)
        evidence_out[j : j + 1, :] = top + jnp.log(first) + shift
        ess_out[j : j + 1, :] = first * first / (second * count)

    @pl.when(z == ROOT)
    def _():
        v_moved.wait_recv()
        best = vbuf[0]
        for k in range(1, NG * NJ):
            best = jnp.maximum(best, vbuf[k])
        best = jnp.max(best)
        mass = jnp.zeros((1, LANE), jnp.float32)
        for k in range(NG * NJ):
            mass += jnp.exp2((vbuf[k] - best) * LOG2E)
        norm = best + jnp.log(jnp.full((1, LANE), jnp.sum(mass)))
        for j in range(NJ):
            pbuf[j : j + 1, :] = vbuf[gi * NJ + j] - norm
        for peer in z_peers:
            remote(pbuf, pbuf, p_send, p_recv, peer)

    for copy in (id_moved, c_moved, z_moved, stats_moved(0), stats_moved(1)):
        copy.wait_send()

    @pl.when(z != ROOT)
    def _():
        moved(lse, l_send, l_recv).wait_send()
        moved(pbuf, p_send, p_recv).wait_recv()

    @pl.when(z == ROOT)
    def _():
        v_moved.wait_send()
        for _ in range(NZ - 1):
            moved(pbuf, p_send, p_recv).wait_send()

    posterior_out[...] = pbuf[...]


def finish(evidence, ess, posterior, evidence_out, ess_out, posterior_out, sem):
    pairs = ((evidence, evidence_out), (ess, ess_out), (posterior, posterior_out))
    copies = [pltpu.make_async_copy(a, b, sem.at[k]) for k, (a, b) in enumerate(pairs)]
    for copy in copies:
        copy.start()
    for copy in copies:
        copy.wait()


def body(summary, weight, offset, prior, event, live):
    rows, bins = summary.shape
    cols = weight.shape[1]
    dma, vmem, smem = pltpu.SemaphoreType.DMA, pltpu.VMEM, pltpu.SMEM
    f32 = jnp.float32
    hbm = pl.BlockSpec(memory_space=pltpu.HBM)
    local = pl.BlockSpec(memory_space=pltpu.VMEM)
    kept = vmem((NJ, LANE), f32)
    outs = pl.pallas_call(
        kernel,
        name="reweight",
        out_shape=(kept, kept, kept),
        in_specs=[hbm] * 6,
        out_specs=(local,) * 3,
        scratch_shapes=[
            vmem((rows, bins), jnp.bfloat16),
            vmem((bins, cols), jnp.bfloat16),
            vmem((2, max(SIZES), cols), f32),
            vmem((TILES, LANE), f32),
            vmem((NJ, LANE), f32),
            smem((TILES,), jnp.int32),
            smem((TILES,), jnp.int32),
            vmem((NY, TILES + 1, 1, LANE), f32),
            vmem((NJ, TILES, 2, LANE), f32),
            vmem((NY, TILES, 2, LANE), f32),
            vmem((3, EVENTS, LANE), f32),
            vmem((EVENTS, LANE), f32),
            vmem((NZ, EVENTS, LANE), f32),
            vmem((EVENTS, 2, LANE), f32),
            vmem((EVENTS, 2, LANE), f32),
            vmem((NZ, 1, LANE), f32),
            vmem((NG * NJ, 1, LANE), f32),
            vmem((NJ, LANE), f32),
            dma((5,)),
            dma((len(SIZES),)),
            dma, dma,
            dma((2,)),
            dma((2,)),
            dma, dma, dma, dma, dma, dma, dma, dma, dma, dma,
            pltpu.SemaphoreType.REGULAR((2,)),
        ],
        compiler_params=pltpu.CompilerParams(
            collective_id=0, has_side_effects=True, vmem_limit_bytes=32 * 1024 * 1024
        ),
        cost_estimate=pl.CostEstimate(
            flops=2 * rows * bins * cols, bytes_accessed=2 * rows * bins, transcendentals=rows * cols
        ),
    )(*(
        pltpu.with_memory_space_constraint(a, pltpu.HBM)
        for a in (summary, weight, prior.reshape(TILES, LANE), offset.reshape(NJ, LANE), event, live)
    ))
    small = jax.ShapeDtypeStruct((NJ, LANE), f32)
    evidence, ess, posterior = pl.pallas_call(
        finish,
        name="finish",
        out_shape=(small, small, small),
        in_specs=[local] * 3,
        out_specs=(hbm,) * 3,
        scratch_shapes=[dma((3,))],
        compiler_params=pltpu.CompilerParams(vmem_limit_bytes=1024 * 1024),
    )(*outs)
    return evidence.reshape(1, cols), ess.reshape(1, cols), posterior.reshape(cols)


def solution(mesh):
    in_specs = (P("samp", None), P(None, "grid"), P("grid"), P("samp"), P("samp"), P("samp"))
    out_specs = (P("samp", "grid"), P("samp", "grid"), P("grid"))
    return jax.shard_map(body, mesh=mesh, in_specs=in_specs, out_specs=out_specs, check_vma=False)
```

```python
import jax
import jax.numpy as jnp
from jax import lax
from jax.experimental import pallas as pl
from jax.experimental.pallas import tpu as pltpu
from jax.sharding import PartitionSpec as P

EVENTS = 64
NX, NC, NY, NZ = 4, 2, 4, 16
NG = NX * NC
TILE = 128
LANE = 128
NJ = 4
TILES = 16
SIZES = (256, 512, 512, 512, 256)
WAITS = 3
ROOT = 0
HOP = 4
BIG = -1e30
LOG2E = 1.4426950408889634
MESH = pl.DeviceIdType.MESH


def kernel(
    summary, weight, prior, offset, event_in, live_in,
    evidence_out, ess_out, posterior_out,
    x_buf, w_buf, scores, prior_buf, offset_buf, event, live,
    yid, ysend, yrecv, held, lse, lse_all, zsend, zrecv, crecv, vbuf,
    in_sem, x_sem, id_send, id_recv, y_send, y_recv, c_send, c_recv, z_send, z_recv,
    l_send, l_recv, v_send, v_recv, r_send, r_recv, known,
):
    gi, si = lax.axis_index("grid"), lax.axis_index("samp")
    x, c = gi // NC, lax.rem(gi, NC)
    z, y = si // NY, lax.rem(si, NY)

    starts = [sum(SIZES[:g]) for g in range(len(SIZES))]
    x_copies = []
    for g, (at, size) in enumerate(zip(starts, SIZES)):
        part = pl.ds(at, size)
        x_copies.append(pltpu.make_async_copy(summary.at[part], x_buf.at[part], x_sem.at[g]))
    pairs = (
        (weight, w_buf), (prior, prior_buf), (event_in, event), (live_in, live), (offset, offset_buf)
    )
    w_copy, *small_copies = [
        pltpu.make_async_copy(a, b, in_sem.at[k]) for k, (a, b) in enumerate(pairs)
    ]
    for copy in (*small_copies, w_copy, *x_copies):
        copy.start()

    y_index = [lax.rem(y + d, NY) for d in range(1, NY)]
    y_peers = [(gi, z * NY + k) for k in y_index]
    z_index = [lax.rem(z + d, NZ) for d in range(1, NZ)]
    z_peers = [(gi, k * NY + y) for k in z_index]
    grid_peers, v_peers = [], []
    for dx in (2, 1, 3, 0):
        for dy in (2, 1, 3, 0):
            for dc in (1, 0):
                grid = lax.rem(x + dx, NX) * NC + lax.rem(c + dc, NC)
                if not dy and (dx or dc):
                    grid_peers.append((grid, si))
                if dx or dc or dy:
                    v_peers.append((grid, z * NY + lax.rem(y + dy, NY)))

    near = y_peers + grid_peers + [z_peers[d - 1] for k in range(1, HOP + 1) for d in (k, NZ - k)]
    barrier = pltpu.get_barrier_semaphore()
    for peer in near:
        pl.semaphore_signal(barrier, inc=1, device_id=peer, device_id_type=MESH)

    lane = lax.broadcasted_iota(jnp.int32, (1, LANE), 1)

    def dot(g):
        if g < WAITS:
            for copy in x_copies[g:] if g == WAITS - 1 else x_copies[g : g + 1]:
                copy.wait()
        scores[g % 2, : SIZES[g], :] = jnp.dot(
            x_buf[starts[g] : starts[g] + SIZES[g], :], w_buf[...],
            preferred_element_type=jnp.float32,
        )

    def stats(g):
        for i in range(SIZES[g] // TILE):
            t = starts[g] // TILE + i
            add = jnp.where(lane < live[t], -prior_buf[t : t + 1, :], BIG)
            add = jnp.transpose(jnp.broadcast_to(add, (LANE, LANE)))
            for j in range(NJ):
                v = scores[g % 2, i * TILE : (i + 1) * TILE, j * LANE : (j + 1) * LANE] + add
                top = jnp.max(v, axis=0, keepdims=True)
                p = jnp.exp2((v - top) * LOG2E)
                first = jnp.sum(p, axis=0, keepdims=True)
                second = jnp.sum(p * p, axis=0, keepdims=True)
                ysend[j, t, 0:1, :] = top + jnp.log(first)
                ysend[j, t, 1:2, :] = second / (first * first)

    def remote(src, dst, send_sem, recv_sem, peer):
        copy = pltpu.make_async_remote_copy(
            src_ref=src, dst_ref=dst, send_sem=send_sem, recv_sem=recv_sem,
            device_id=peer, device_id_type=MESH,
        )
        copy.start()

    def moved(ref, send_sem, recv_sem):
        return pltpu.make_async_remote_copy(
            src_ref=ref, dst_ref=ref, send_sem=send_sem, recv_sem=recv_sem,
            device_id=y_peers[0], device_id_type=MESH,
        )

    id_moved = moved(yid.at[pl.ds(0, NY - 1)], id_send, id_recv)
    c_moved = moved(crecv.at[pl.ds(0, NZ - 1)], c_send, c_recv)
    z_moved = moved(zrecv.at[pl.ds(0, EVENTS - 1)], z_send, z_recv)

    split = starts[-1] // TILE
    batches = (pl.ds(0, split), pl.ds(split, TILES - split))

    def send_stats(b):
        for k, peer in zip(y_index, y_peers):
            remote(
                ysend.at[k, batches[b]], yrecv.at[y, batches[b]], y_send.at[b], y_recv.at[b], peer
            )

    def stats_moved(b):
        size = TILES - split if b else split
        return moved(yrecv.at[pl.ds(0, NY - 1), pl.ds(0, size)], y_send.at[b], y_recv.at[b])

    def got_stats(b):
        yrecv[y, batches[b]] = ysend[y, batches[b]]
        stats_moved(b).wait_recv()

    for copy in small_copies:
        copy.wait()
    count = jnp.zeros((1, LANE), jnp.float32)
    for t in range(TILES):
        yid[y, t] = jnp.full((1, LANE), event[t].astype(jnp.float32))
        count += jnp.where(lane == event[t], live[t].astype(jnp.float32), 0.0)
    yid[y, TILES] = count
    w_copy.wait()
    dot(0)
    for g in range(1, len(SIZES)):
        dot(g)
        stats(g - 1)
    pl.semaphore_wait(barrier, len(near))
    for peer in y_peers:
        remote(yid.at[y], yid.at[y], id_send, id_recv, peer)
    send_stats(0)
    for d in (HOP, NZ - HOP):
        pl.semaphore_signal(known.at[0], inc=1, device_id=z_peers[d - 1], device_id_type=MESH)
    stats(len(SIZES) - 1)
    send_stats(1)

    id_moved.wait_recv()
    count = yid[0, TILES]
    for s in range(1, NY):
        count += yid[s, TILES]
    crecv[z] = count
    index = lax.broadcasted_iota(jnp.int32, (EVENTS, LANE), 0).astype(jnp.float32)

    def chosen(s, t):
        member = jnp.broadcast_to(yid[s, t], (EVENTS, LANE)) == index
        return jnp.where(member, yrecv[s, t, 0:1, :], BIG)

    def merged(order, top, first, second):
        high = top
        for entry in order:
            high = jnp.maximum(high, chosen(*entry))
        keep = jnp.exp2((top - high) * LOG2E)
        first, second = first * keep, second * (keep * keep)
        for s, t in order:
            w = jnp.exp2((chosen(s, t) - high) * LOG2E)
            first += w
            second += w * w * yrecv[s, t, 1:2, :]
        return high, first, second

    zero = jnp.zeros((EVENTS, LANE), jnp.float32)
    got_stats(0)
    order = [(s, t) for t in range(split) for s in range(NY)]
    held[0], held[1], held[2] = merged(order, zero + BIG, zero, zero)
    pl.semaphore_wait(known.at[0], 2)
    for peer in y_peers:
        pl.semaphore_signal(known.at[1], inc=1, device_id=peer, device_id_type=MESH)
    for peer in z_peers:
        remote(crecv.at[z], crecv.at[z], c_send, c_recv, peer)
    got_stats(1)
    order = [(s, t) for t in range(split, TILES) for s in range(NY)]
    top, first, second = merged(order, held[0], held[1], held[2])
    lse[...] = top + jnp.log(first)

    @pl.when(z != ROOT)
    def _():
        remote(lse, lse_all.at[z], l_send, l_recv, (gi, ROOT * NY + y))

    ratio = second / (first * first)
    for k in range(EVENTS):
        zsend[k, 0:1, :] = lse[k : k + 1, :]
        zsend[k, 1:2, :] = ratio[k : k + 1, :]
    zrecv[si] = zsend[si]
    pl.semaphore_wait(known.at[1], NY - 1)
    c_moved.wait_recv()
    for dz in sorted(range(NZ), key=lambda d: abs(d - NZ // 2)):
        for dy in range(NY):
            if dz or dy:
                k = lax.rem(z + dz, NZ) * NY + lax.rem(y + dy, NY)
                remote(zsend.at[k], zrecv.at[si], z_send, z_recv, (gi, k))

    count = crecv[0]
    for k in range(1, NZ):
        count += crecv[k]
    own = gi * NJ + y
    v_moved = moved(vbuf.at[pl.ds(0, NG * NJ - 1)], v_send, v_recv)
    row_moved = moved(vbuf.at[0], r_send, r_recv)

    def send_plane():
        for peer in v_peers:
            remote(vbuf.at[own], vbuf.at[own], v_send, v_recv, peer)


    @pl.when(z == ROOT)
    def _():
        logs = jnp.sum(jnp.where(lane < EVENTS, jnp.log(jnp.maximum(count, 1.0)), 0.0))
        lse_all[ROOT] = lse[...]
        moved(lse_all.at[pl.ds(0, NZ - 1)], l_send, l_recv).wait_recv()
        top = lse_all[0]
        for k in range(1, NZ):
            top = jnp.maximum(top, lse_all[k])
        first = jnp.zeros((EVENTS, LANE), jnp.float32)
        for k in range(NZ):
            first += jnp.exp2((lse_all[k] - top) * LOG2E)
        line = jnp.sum(top + jnp.log(first), axis=0, keepdims=True)
        vbuf[own] = (line - logs) * (1.0 / EVENTS) + offset_buf[pl.ds(y, 1), :]
        send_plane()
        for d in sorted(range(1, NZ), key=lambda d: abs(d - NZ // 2)):
            remote(vbuf.at[own], vbuf.at[own], r_send, r_recv, z_peers[d - 1])

    @pl.when(z != ROOT)
    def _():
        row_moved.wait_recv()
        send_plane()

    count = jnp.full((1, LANE), jnp.sum(jnp.where(lane == si, count, 0.0)))
    z_moved.wait_recv()
    for j in range(NJ):
        top = zrecv[j, 0:1, :]
        for k in range(1, NZ):
            top = jnp.maximum(top, zrecv[k * NY + j, 0:1, :])
        first = jnp.zeros((1, LANE), jnp.float32)
        second = jnp.zeros((1, LANE), jnp.float32)
        for k in range(NZ):
            w = jnp.exp2((zrecv[k * NY + j, 0:1, :] - top) * LOG2E)
            first += w
            second += w * w * zrecv[k * NY + j, 1:2, :]
        shift = offset_buf[j : j + 1, :] - jnp.log(count)
        evidence_out[j : j + 1, :] = top + jnp.log(first) + shift
        ess_out[j : j + 1, :] = first * first / (second * count)

    v_moved.wait_recv()
    best = vbuf[0]
    for k in range(1, NG * NJ):
        best = jnp.maximum(best, vbuf[k])
    best = jnp.max(best)
    mass = jnp.zeros((1, LANE), jnp.float32)
    for k in range(NG * NJ):
        mass += jnp.exp2((vbuf[k] - best) * LOG2E)
    norm = best + jnp.log(jnp.full((1, LANE), jnp.sum(mass)))
    for j in range(NJ):
        posterior_out[j : j + 1, :] = vbuf[gi * NJ + j] - norm

    for copy in (id_moved, c_moved, z_moved, v_moved, stats_moved(0), stats_moved(1)):
        copy.wait_send()

    @pl.when(z != ROOT)
    def _():
        moved(lse, l_send, l_recv).wait_send()

    @pl.when(z == ROOT)
    def _():
        moved(vbuf.at[pl.ds(0, NZ - 1)], r_send, r_recv).wait_send()


def finish(evidence, ess, posterior, evidence_out, ess_out, posterior_out, sem):
    pairs = ((evidence, evidence_out), (ess, ess_out), (posterior, posterior_out))
    copies = [pltpu.make_async_copy(a, b, sem.at[k]) for k, (a, b) in enumerate(pairs)]
    for copy in copies:
        copy.start()
    for copy in copies:
        copy.wait()


def body(summary, weight, offset, prior, event, live):
    rows, bins = summary.shape
    cols = weight.shape[1]
    dma, vmem, smem = pltpu.SemaphoreType.DMA, pltpu.VMEM, pltpu.SMEM
    f32 = jnp.float32
    hbm = pl.BlockSpec(memory_space=pltpu.HBM)
    local = pl.BlockSpec(memory_space=pltpu.VMEM)
    kept = vmem((NJ, LANE), f32)
    outs = pl.pallas_call(
        kernel,
        name="reweight",
        out_shape=(kept, kept, kept),
        in_specs=[hbm] * 6,
        out_specs=(local,) * 3,
        scratch_shapes=[
            vmem((rows, bins), jnp.bfloat16),
            vmem((bins, cols), jnp.bfloat16),
            vmem((2, max(SIZES), cols), f32),
            vmem((TILES, LANE), f32),
            vmem((NJ, LANE), f32),
            smem((TILES,), jnp.int32),
            smem((TILES,), jnp.int32),
            vmem((NY, TILES + 1, 1, LANE), f32),
            vmem((NJ, TILES, 2, LANE), f32),
            vmem((NY, TILES, 2, LANE), f32),
            vmem((3, EVENTS, LANE), f32),
            vmem((EVENTS, LANE), f32),
            vmem((NZ, EVENTS, LANE), f32),
            vmem((EVENTS, 2, LANE), f32),
            vmem((EVENTS, 2, LANE), f32),
            vmem((NZ, 1, LANE), f32),
            vmem((NG * NJ, 1, LANE), f32),
            dma((5,)),
            dma((len(SIZES),)),
            dma, dma,
            dma((2,)),
            dma((2,)),
            dma, dma, dma, dma, dma, dma, dma, dma, dma, dma,
            pltpu.SemaphoreType.REGULAR((2,)),
        ],
        compiler_params=pltpu.CompilerParams(
            collective_id=0, has_side_effects=True, vmem_limit_bytes=32 * 1024 * 1024
        ),
        cost_estimate=pl.CostEstimate(
            flops=2 * rows * bins * cols, bytes_accessed=2 * rows * bins, transcendentals=rows * cols
        ),
    )(*(
        pltpu.with_memory_space_constraint(a, pltpu.HBM)
        for a in (summary, weight, prior.reshape(TILES, LANE), offset.reshape(NJ, LANE), event, live)
    ))
    small = jax.ShapeDtypeStruct((NJ, LANE), f32)
    evidence, ess, posterior = pl.pallas_call(
        finish,
        name="finish",
        out_shape=(small, small, small),
        in_specs=[local] * 3,
        out_specs=(hbm,) * 3,
        scratch_shapes=[dma((3,))],
        compiler_params=pltpu.CompilerParams(vmem_limit_bytes=1024 * 1024),
    )(*outs)
    return evidence.reshape(1, cols), ess.reshape(1, cols), posterior.reshape(cols)


def solution(mesh):
    in_specs = (P("samp", None), P(None, "grid"), P("grid"), P("samp"), P("samp"), P("samp"))
    out_specs = (P("samp", "grid"), P("samp", "grid"), P("grid"))
    return jax.shard_map(body, mesh=mesh, in_specs=in_specs, out_specs=out_specs, check_vma=False)
```

```python
import jax
import jax.numpy as jnp
from jax import lax
from jax.experimental import pallas as pl
from jax.experimental.pallas import tpu as pltpu
from jax.sharding import PartitionSpec as P

EVENTS = 64
NX, NC, NY, NZ = 4, 2, 4, 16
NG = NX * NC
TILE = 128
LANE = 128
NJ = 4
TILES = 16
SIZES = (256, 512, 512, 512, 256)
WAITS = 3
ROOT = 0
DIRECT = 4
HOP = 4
BIG = -1e30
LOG2E = 1.4426950408889634
MESH = pl.DeviceIdType.MESH


def kernel(
    summary, weight, prior, offset, event_in, live_in,
    evidence_out, ess_out, posterior_out,
    x_buf, w_buf, scores, prior_buf, offset_buf, event, live,
    yid, ysend, yrecv, held, lse, lse_all, zsend, zrecv, crecv, vbuf,
    in_sem, x_sem, id_send, id_recv, y_send, y_recv, c_send, c_recv, z_send, z_recv,
    l_send, l_recv, v_send, v_recv, r_send, r_recv, d_send, d_recv, known,
):
    gi, si = lax.axis_index("grid"), lax.axis_index("samp")
    x, c = gi // NC, lax.rem(gi, NC)
    z, y = si // NY, lax.rem(si, NY)

    starts = [sum(SIZES[:g]) for g in range(len(SIZES))]
    x_copies = []
    for g, (at, size) in enumerate(zip(starts, SIZES)):
        part = pl.ds(at, size)
        x_copies.append(pltpu.make_async_copy(summary.at[part], x_buf.at[part], x_sem.at[g]))
    pairs = (
        (weight, w_buf), (prior, prior_buf), (event_in, event), (live_in, live), (offset, offset_buf)
    )
    w_copy, *small_copies = [
        pltpu.make_async_copy(a, b, in_sem.at[k]) for k, (a, b) in enumerate(pairs)
    ]
    for copy in (*small_copies, w_copy, *x_copies):
        copy.start()

    y_index = [lax.rem(y + d, NY) for d in range(1, NY)]
    y_peers = [(gi, z * NY + k) for k in y_index]
    z_index = [lax.rem(z + d, NZ) for d in range(1, NZ)]
    z_peers = [(gi, k * NY + y) for k in z_index]
    grid_peers, v_peers = [], []
    for dx in (2, 1, 3, 0):
        for dy in (2, 1, 3, 0):
            for dc in (1, 0):
                grid = lax.rem(x + dx, NX) * NC + lax.rem(c + dc, NC)
                if not dy and (dx or dc):
                    grid_peers.append((grid, si))
                if dx or dc or dy:
                    v_peers.append((grid, z * NY + lax.rem(y + dy, NY)))

    near = y_peers + grid_peers + [z_peers[d - 1] for k in range(1, HOP + 1) for d in (k, NZ - k)]
    barrier = pltpu.get_barrier_semaphore()
    for peer in near:
        pl.semaphore_signal(barrier, inc=1, device_id=peer, device_id_type=MESH)

    lane = lax.broadcasted_iota(jnp.int32, (1, LANE), 1)

    def dot(g):
        if g < WAITS:
            for copy in x_copies[g:] if g == WAITS - 1 else x_copies[g : g + 1]:
                copy.wait()
        scores[g % 2, : SIZES[g], :] = jnp.dot(
            x_buf[starts[g] : starts[g] + SIZES[g], :], w_buf[...],
            preferred_element_type=jnp.float32,
        )

    def stats(g):
        for i in range(SIZES[g] // TILE):
            t = starts[g] // TILE + i
            add = jnp.where(lane < live[t], -prior_buf[t : t + 1, :], BIG)
            add = jnp.transpose(jnp.broadcast_to(add, (LANE, LANE)))
            for j in range(NJ):
                v = scores[g % 2, i * TILE : (i + 1) * TILE, j * LANE : (j + 1) * LANE] + add
                top = jnp.max(v, axis=0, keepdims=True)
                p = jnp.exp2((v - top) * LOG2E)
                first = jnp.sum(p, axis=0, keepdims=True)
                second = jnp.sum(p * p, axis=0, keepdims=True)
                ysend[j, t, 0:1, :] = top + jnp.log(first)
                ysend[j, t, 1:2, :] = second / (first * first)

    def remote(src, dst, send_sem, recv_sem, peer):
        copy = pltpu.make_async_remote_copy(
            src_ref=src, dst_ref=dst, send_sem=send_sem, recv_sem=recv_sem,
            device_id=peer, device_id_type=MESH,
        )
        copy.start()

    def moved(ref, send_sem, recv_sem):
        return pltpu.make_async_remote_copy(
            src_ref=ref, dst_ref=ref, send_sem=send_sem, recv_sem=recv_sem,
            device_id=y_peers[0], device_id_type=MESH,
        )

    id_moved = moved(yid.at[pl.ds(0, NY - 1)], id_send, id_recv)
    c_moved = moved(crecv.at[pl.ds(0, NZ - 1)], c_send, c_recv)
    z_moved = moved(zrecv.at[pl.ds(0, EVENTS - 1)], z_send, z_recv)

    split = starts[-1] // TILE
    batches = (pl.ds(0, split), pl.ds(split, TILES - split))

    def send_stats(b):
        for k, peer in zip(y_index, y_peers):
            remote(
                ysend.at[k, batches[b]], yrecv.at[y, batches[b]], y_send.at[b], y_recv.at[b], peer
            )

    def stats_moved(b):
        size = TILES - split if b else split
        return moved(yrecv.at[pl.ds(0, NY - 1), pl.ds(0, size)], y_send.at[b], y_recv.at[b])

    def got_stats(b):
        yrecv[y, batches[b]] = ysend[y, batches[b]]
        stats_moved(b).wait_recv()

    for copy in small_copies:
        copy.wait()
    count = jnp.zeros((1, LANE), jnp.float32)
    for t in range(TILES):
        yid[y, t] = jnp.full((1, LANE), event[t].astype(jnp.float32))
        count += jnp.where(lane == event[t], live[t].astype(jnp.float32), 0.0)
    yid[y, TILES] = count
    w_copy.wait()
    dot(0)
    for g in range(1, len(SIZES)):
        dot(g)
        stats(g - 1)
    pl.semaphore_wait(barrier, len(near))
    for peer in y_peers:
        remote(yid.at[y], yid.at[y], id_send, id_recv, peer)
    send_stats(0)
    for d in (HOP, NZ - HOP):
        pl.semaphore_signal(known.at[0], inc=1, device_id=z_peers[d - 1], device_id_type=MESH)
    stats(len(SIZES) - 1)
    send_stats(1)

    id_moved.wait_recv()
    count = yid[0, TILES]
    for s in range(1, NY):
        count += yid[s, TILES]
    crecv[z] = count
    index = lax.broadcasted_iota(jnp.int32, (EVENTS, LANE), 0).astype(jnp.float32)

    def chosen(s, t):
        member = jnp.broadcast_to(yid[s, t], (EVENTS, LANE)) == index
        return jnp.where(member, yrecv[s, t, 0:1, :], BIG)

    def merged(order, top, first, second):
        high = top
        for entry in order:
            high = jnp.maximum(high, chosen(*entry))
        keep = jnp.exp2((top - high) * LOG2E)
        first, second = first * keep, second * (keep * keep)
        for s, t in order:
            w = jnp.exp2((chosen(s, t) - high) * LOG2E)
            first += w
            second += w * w * yrecv[s, t, 1:2, :]
        return high, first, second

    zero = jnp.zeros((EVENTS, LANE), jnp.float32)
    got_stats(0)
    order = [(s, t) for t in range(split) for s in range(NY)]
    held[0], held[1], held[2] = merged(order, zero + BIG, zero, zero)
    pl.semaphore_wait(known.at[0], 2)
    for peer in y_peers:
        pl.semaphore_signal(known.at[1], inc=1, device_id=peer, device_id_type=MESH)
    for peer in z_peers:
        remote(crecv.at[z], crecv.at[z], c_send, c_recv, peer)
    got_stats(1)
    order = [(s, t) for t in range(split, TILES) for s in range(NY)]
    top, first, second = merged(order, held[0], held[1], held[2])
    lse[...] = top + jnp.log(first)

    @pl.when(z != ROOT)
    def _():
        remote(lse, lse_all.at[z], l_send, l_recv, (gi, ROOT * NY + y))

    ratio = second / (first * first)
    for k in range(EVENTS):
        zsend[k, 0:1, :] = lse[k : k + 1, :]
        zsend[k, 1:2, :] = ratio[k : k + 1, :]
    zrecv[si] = zsend[si]
    pl.semaphore_wait(known.at[1], NY - 1)
    c_moved.wait_recv()
    for dz in sorted(range(NZ), key=lambda d: abs(d - NZ // 2)):
        for dy in range(NY):
            if dz or dy:
                k = lax.rem(z + dz, NZ) * NY + lax.rem(y + dy, NY)
                remote(zsend.at[k], zrecv.at[si], z_send, z_recv, (gi, k))

    count = crecv[0]
    for k in range(1, NZ):
        count += crecv[k]
    own = gi * NJ + y
    v_moved = moved(vbuf.at[pl.ds(0, NG * NJ - 1)], v_send, v_recv)
    row_moved = moved(vbuf.at[0], r_send, r_recv)

    def send_plane(target, peers, send_sem, recv_sem):
        for grid, samp in peers:
            samp = target * NY + lax.rem(samp, NY)
            remote(vbuf.at[own], vbuf.at[own], send_sem, recv_sem, (grid, samp))


    @pl.when(z == ROOT)
    def _():
        logs = jnp.sum(jnp.where(lane < EVENTS, jnp.log(jnp.maximum(count, 1.0)), 0.0))
        lse_all[ROOT] = lse[...]
        moved(lse_all.at[pl.ds(0, NZ - 1)], l_send, l_recv).wait_recv()
        top = lse_all[0]
        for k in range(1, NZ):
            top = jnp.maximum(top, lse_all[k])
        first = jnp.zeros((EVENTS, LANE), jnp.float32)
        for k in range(NZ):
            first += jnp.exp2((lse_all[k] - top) * LOG2E)
        line = jnp.sum(top + jnp.log(first), axis=0, keepdims=True)
        vbuf[own] = (line - logs) * (1.0 / EVENTS) + offset_buf[pl.ds(y, 1), :]
        send_plane(ROOT, v_peers, v_send, v_recv)
        send_plane(ROOT + 1, [*v_peers, (gi, si)], d_send, d_recv)
        for d in range(DIRECT, NZ):
            remote(vbuf.at[own], vbuf.at[own], r_send, r_recv, z_peers[d - 1])
        for target in range(ROOT + 2, ROOT + DIRECT):
            send_plane(target, [*v_peers, (gi, si)], d_send, d_recv)

    @pl.when(z >= DIRECT)
    def _():
        row_moved.wait_recv()
        send_plane(z, v_peers, v_send, v_recv)

    count = jnp.full((1, LANE), jnp.sum(jnp.where(lane == si, count, 0.0)))
    z_moved.wait_recv()
    for j in range(NJ):
        top = zrecv[j, 0:1, :]
        for k in range(1, NZ):
            top = jnp.maximum(top, zrecv[k * NY + j, 0:1, :])
        first = jnp.zeros((1, LANE), jnp.float32)
        second = jnp.zeros((1, LANE), jnp.float32)
        for k in range(NZ):
            w = jnp.exp2((zrecv[k * NY + j, 0:1, :] - top) * LOG2E)
            first += w
            second += w * w * zrecv[k * NY + j, 1:2, :]
        shift = offset_buf[j : j + 1, :] - jnp.log(count)
        evidence_out[j : j + 1, :] = top + jnp.log(first) + shift
        ess_out[j : j + 1, :] = first * first / (second * count)

    @pl.when((z > ROOT) & (z < DIRECT))
    def _():
        moved(vbuf, d_send, d_recv).wait_recv()

    @pl.when((z == ROOT) | (z >= DIRECT))
    def _():
        v_moved.wait_recv()

    best = vbuf[0]
    for k in range(1, NG * NJ):
        best = jnp.maximum(best, vbuf[k])
    best = jnp.max(best)
    mass = jnp.zeros((1, LANE), jnp.float32)
    for k in range(NG * NJ):
        mass += jnp.exp2((vbuf[k] - best) * LOG2E)
    norm = best + jnp.log(jnp.full((1, LANE), jnp.sum(mass)))
    for j in range(NJ):
        posterior_out[j : j + 1, :] = vbuf[gi * NJ + j] - norm

    for copy in (id_moved, c_moved, z_moved, stats_moved(0), stats_moved(1)):
        copy.wait_send()

    @pl.when(z != ROOT)
    def _():
        moved(lse, l_send, l_recv).wait_send()

    @pl.when(z == ROOT)
    def _():
        moved(vbuf.at[pl.ds(0, NZ - DIRECT)], r_send, r_recv).wait_send()
        rows = zrecv.at[pl.ds(0, (DIRECT - 1) * NG * NJ // 2)]
        moved(rows, d_send, d_recv).wait_send()

    @pl.when((z == ROOT) | (z >= DIRECT))
    def _():
        v_moved.wait_send()


def finish(evidence, ess, posterior, evidence_out, ess_out, posterior_out, sem):
    pairs = ((evidence, evidence_out), (ess, ess_out), (posterior, posterior_out))
    copies = [pltpu.make_async_copy(a, b, sem.at[k]) for k, (a, b) in enumerate(pairs)]
    for copy in copies:
        copy.start()
    for copy in copies:
        copy.wait()


def body(summary, weight, offset, prior, event, live):
    rows, bins = summary.shape
    cols = weight.shape[1]
    dma, vmem, smem = pltpu.SemaphoreType.DMA, pltpu.VMEM, pltpu.SMEM
    f32 = jnp.float32
    hbm = pl.BlockSpec(memory_space=pltpu.HBM)
    local = pl.BlockSpec(memory_space=pltpu.VMEM)
    kept = vmem((NJ, LANE), f32)
    outs = pl.pallas_call(
        kernel,
        name="reweight",
        out_shape=(kept, kept, kept),
        in_specs=[hbm] * 6,
        out_specs=(local,) * 3,
        scratch_shapes=[
            vmem((rows, bins), jnp.bfloat16),
            vmem((bins, cols), jnp.bfloat16),
            vmem((2, max(SIZES), cols), f32),
            vmem((TILES, LANE), f32),
            vmem((NJ, LANE), f32),
            smem((TILES,), jnp.int32),
            smem((TILES,), jnp.int32),
            vmem((NY, TILES + 1, 1, LANE), f32),
            vmem((NJ, TILES, 2, LANE), f32),
            vmem((NY, TILES, 2, LANE), f32),
            vmem((3, EVENTS, LANE), f32),
            vmem((EVENTS, LANE), f32),
            vmem((NZ, EVENTS, LANE), f32),
            vmem((EVENTS, 2, LANE), f32),
            vmem((EVENTS, 2, LANE), f32),
            vmem((NZ, 1, LANE), f32),
            vmem((NG * NJ, 1, LANE), f32),
            dma((5,)),
            dma((len(SIZES),)),
            dma, dma,
            dma((2,)),
            dma((2,)),
            dma, dma, dma, dma, dma, dma, dma, dma, dma, dma, dma, dma,
            pltpu.SemaphoreType.REGULAR((2,)),
        ],
        compiler_params=pltpu.CompilerParams(
            collective_id=0, has_side_effects=True, vmem_limit_bytes=32 * 1024 * 1024
        ),
        cost_estimate=pl.CostEstimate(
            flops=2 * rows * bins * cols, bytes_accessed=2 * rows * bins, transcendentals=rows * cols
        ),
    )(*(
        pltpu.with_memory_space_constraint(a, pltpu.HBM)
        for a in (summary, weight, prior.reshape(TILES, LANE), offset.reshape(NJ, LANE), event, live)
    ))
    small = jax.ShapeDtypeStruct((NJ, LANE), f32)
    evidence, ess, posterior = pl.pallas_call(
        finish,
        name="finish",
        out_shape=(small, small, small),
        in_specs=[local] * 3,
        out_specs=(hbm,) * 3,
        scratch_shapes=[dma((3,))],
        compiler_params=pltpu.CompilerParams(vmem_limit_bytes=1024 * 1024),
    )(*outs)
    return evidence.reshape(1, cols), ess.reshape(1, cols), posterior.reshape(cols)


def solution(mesh):
    in_specs = (P("samp", None), P(None, "grid"), P("grid"), P("samp"), P("samp"), P("samp"))
    out_specs = (P("samp", "grid"), P("samp", "grid"), P("grid"))
    return jax.shard_map(body, mesh=mesh, in_specs=in_specs, out_specs=out_specs, check_vma=False)
```

```python
import jax
import jax.numpy as jnp
from jax import lax
from jax.experimental import pallas as pl
from jax.experimental.pallas import tpu as pltpu
from jax.sharding import PartitionSpec as P

EVENTS = 64
NX, NC, NY, NZ = 4, 2, 4, 16
NG = NX * NC
TILE = 128
LANE = 128
NJ = 4
TILES = 16
SIZES = (256, 512, 512, 512, 256)
WAITS = 3
ROOT = 0
DIRECT = 5
HOP = 4
BIG = -1e30
LOG2E = 1.4426950408889634
MESH = pl.DeviceIdType.MESH


def kernel(
    summary, weight, prior, offset, event_in, live_in,
    evidence_out, ess_out, posterior_out,
    x_buf, w_buf, scores, prior_buf, offset_buf, event, live,
    yid, ysend, yrecv, held, lse, lse_all, zsend, zrecv, crecv, vbuf,
    in_sem, x_sem, id_send, id_recv, y_send, y_recv, c_send, c_recv, z_send, z_recv,
    l_send, l_recv, v_send, v_recv, r_send, r_recv, d_send, d_recv, known,
):
    gi, si = lax.axis_index("grid"), lax.axis_index("samp")
    x, c = gi // NC, lax.rem(gi, NC)
    z, y = si // NY, lax.rem(si, NY)

    starts = [sum(SIZES[:g]) for g in range(len(SIZES))]
    x_copies = []
    for g, (at, size) in enumerate(zip(starts, SIZES)):
        part = pl.ds(at, size)
        x_copies.append(pltpu.make_async_copy(summary.at[part], x_buf.at[part], x_sem.at[g]))
    pairs = (
        (weight, w_buf), (prior, prior_buf), (event_in, event), (live_in, live), (offset, offset_buf)
    )
    w_copy, *small_copies = [
        pltpu.make_async_copy(a, b, in_sem.at[k]) for k, (a, b) in enumerate(pairs)
    ]
    for copy in (*small_copies, w_copy, *x_copies):
        copy.start()

    y_index = [lax.rem(y + d, NY) for d in range(1, NY)]
    y_peers = [(gi, z * NY + k) for k in y_index]
    z_index = [lax.rem(z + d, NZ) for d in range(1, NZ)]
    z_peers = [(gi, k * NY + y) for k in z_index]
    grid_peers, v_peers = [], []
    for dx in (2, 1, 3, 0):
        for dy in (2, 1, 3, 0):
            for dc in (1, 0):
                grid = lax.rem(x + dx, NX) * NC + lax.rem(c + dc, NC)
                if not dy and (dx or dc):
                    grid_peers.append((grid, si))
                if dx or dc or dy:
                    v_peers.append((grid, z * NY + lax.rem(y + dy, NY)))

    near = y_peers + grid_peers + [z_peers[d - 1] for k in range(1, HOP + 1) for d in (k, NZ - k)]
    barrier = pltpu.get_barrier_semaphore()
    for peer in near:
        pl.semaphore_signal(barrier, inc=1, device_id=peer, device_id_type=MESH)

    lane = lax.broadcasted_iota(jnp.int32, (1, LANE), 1)

    def dot(g):
        if g < WAITS:
            for copy in x_copies[g:] if g == WAITS - 1 else x_copies[g : g + 1]:
                copy.wait()
        scores[g % 2, : SIZES[g], :] = jnp.dot(
            x_buf[starts[g] : starts[g] + SIZES[g], :], w_buf[...],
            preferred_element_type=jnp.float32,
        )

    def stats(g):
        for i in range(SIZES[g] // TILE):
            t = starts[g] // TILE + i
            add = jnp.where(lane < live[t], -prior_buf[t : t + 1, :], BIG)
            add = jnp.transpose(jnp.broadcast_to(add, (LANE, LANE)))
            for j in range(NJ):
                v = scores[g % 2, i * TILE : (i + 1) * TILE, j * LANE : (j + 1) * LANE] + add
                top = jnp.max(v, axis=0, keepdims=True)
                p = jnp.exp2((v - top) * LOG2E)
                first = jnp.sum(p, axis=0, keepdims=True)
                second = jnp.sum(p * p, axis=0, keepdims=True)
                ysend[j, t, 0:1, :] = top + jnp.log(first)
                ysend[j, t, 1:2, :] = second / (first * first)

    def remote(src, dst, send_sem, recv_sem, peer):
        copy = pltpu.make_async_remote_copy(
            src_ref=src, dst_ref=dst, send_sem=send_sem, recv_sem=recv_sem,
            device_id=peer, device_id_type=MESH,
        )
        copy.start()

    def moved(ref, send_sem, recv_sem):
        return pltpu.make_async_remote_copy(
            src_ref=ref, dst_ref=ref, send_sem=send_sem, recv_sem=recv_sem,
            device_id=y_peers[0], device_id_type=MESH,
        )

    id_moved = moved(yid.at[pl.ds(0, NY - 1)], id_send, id_recv)
    c_moved = moved(crecv.at[pl.ds(0, NZ - 1)], c_send, c_recv)
    z_moved = moved(zrecv.at[pl.ds(0, EVENTS - 1)], z_send, z_recv)

    split = starts[-1] // TILE
    batches = (pl.ds(0, split), pl.ds(split, TILES - split))

    def send_stats(b):
        for k, peer in zip(y_index, y_peers):
            remote(
                ysend.at[k, batches[b]], yrecv.at[y, batches[b]], y_send.at[b], y_recv.at[b], peer
            )

    def stats_moved(b):
        size = TILES - split if b else split
        return moved(yrecv.at[pl.ds(0, NY - 1), pl.ds(0, size)], y_send.at[b], y_recv.at[b])

    def got_stats(b):
        yrecv[y, batches[b]] = ysend[y, batches[b]]
        stats_moved(b).wait_recv()

    for copy in small_copies:
        copy.wait()
    count = jnp.zeros((1, LANE), jnp.float32)
    for t in range(TILES):
        yid[y, t] = jnp.full((1, LANE), event[t].astype(jnp.float32))
        count += jnp.where(lane == event[t], live[t].astype(jnp.float32), 0.0)
    yid[y, TILES] = count
    w_copy.wait()
    dot(0)
    for g in range(1, len(SIZES)):
        dot(g)
        stats(g - 1)
    pl.semaphore_wait(barrier, len(near))
    for peer in y_peers:
        remote(yid.at[y], yid.at[y], id_send, id_recv, peer)
    send_stats(0)
    for d in (HOP, NZ - HOP):
        pl.semaphore_signal(known.at[0], inc=1, device_id=z_peers[d - 1], device_id_type=MESH)
    stats(len(SIZES) - 1)
    send_stats(1)

    id_moved.wait_recv()
    count = yid[0, TILES]
    for s in range(1, NY):
        count += yid[s, TILES]
    crecv[z] = count
    index = lax.broadcasted_iota(jnp.int32, (EVENTS, LANE), 0).astype(jnp.float32)

    def chosen(s, t):
        member = jnp.broadcast_to(yid[s, t], (EVENTS, LANE)) == index
        return jnp.where(member, yrecv[s, t, 0:1, :], BIG)

    def merged(order, top, first, second):
        high = top
        for entry in order:
            high = jnp.maximum(high, chosen(*entry))
        keep = jnp.exp2((top - high) * LOG2E)
        first, second = first * keep, second * (keep * keep)
        for s, t in order:
            w = jnp.exp2((chosen(s, t) - high) * LOG2E)
            first += w
            second += w * w * yrecv[s, t, 1:2, :]
        return high, first, second

    zero = jnp.zeros((EVENTS, LANE), jnp.float32)
    got_stats(0)
    order = [(s, t) for t in range(split) for s in range(NY)]
    held[0], held[1], held[2] = merged(order, zero + BIG, zero, zero)
    pl.semaphore_wait(known.at[0], 2)
    for peer in y_peers:
        pl.semaphore_signal(known.at[1], inc=1, device_id=peer, device_id_type=MESH)
    for peer in z_peers:
        remote(crecv.at[z], crecv.at[z], c_send, c_recv, peer)
    got_stats(1)
    order = [(s, t) for t in range(split, TILES) for s in range(NY)]
    top, first, second = merged(order, held[0], held[1], held[2])
    lse[...] = top + jnp.log(first)

    @pl.when(z != ROOT)
    def _():
        remote(lse, lse_all.at[z], l_send, l_recv, (gi, ROOT * NY + y))

    ratio = second / (first * first)
    for k in range(EVENTS):
        zsend[k, 0:1, :] = lse[k : k + 1, :]
        zsend[k, 1:2, :] = ratio[k : k + 1, :]
    zrecv[si] = zsend[si]
    pl.semaphore_wait(known.at[1], NY - 1)
    c_moved.wait_recv()
    for dz in sorted(range(NZ), key=lambda d: abs(d - NZ // 2)):
        for dy in range(NY):
            if dz or dy:
                k = lax.rem(z + dz, NZ) * NY + lax.rem(y + dy, NY)
                remote(zsend.at[k], zrecv.at[si], z_send, z_recv, (gi, k))

    count = crecv[0]
    for k in range(1, NZ):
        count += crecv[k]
    own = gi * NJ + y
    v_moved = moved(vbuf.at[pl.ds(0, NG * NJ - 1)], v_send, v_recv)
    row_moved = moved(vbuf.at[0], r_send, r_recv)

    def send_plane(target, peers, send_sem, recv_sem):
        for grid, samp in peers:
            samp = target * NY + lax.rem(samp, NY)
            remote(vbuf.at[own], vbuf.at[own], send_sem, recv_sem, (grid, samp))


    @pl.when(z == ROOT)
    def _():
        logs = jnp.sum(jnp.where(lane < EVENTS, jnp.log(jnp.maximum(count, 1.0)), 0.0))
        lse_all[ROOT] = lse[...]
        moved(lse_all.at[pl.ds(0, NZ - 1)], l_send, l_recv).wait_recv()
        top = lse_all[0]
        for k in range(1, NZ):
            top = jnp.maximum(top, lse_all[k])
        first = jnp.zeros((EVENTS, LANE), jnp.float32)
        for k in range(NZ):
            first += jnp.exp2((lse_all[k] - top) * LOG2E)
        line = jnp.sum(top + jnp.log(first), axis=0, keepdims=True)
        vbuf[own] = (line - logs) * (1.0 / EVENTS) + offset_buf[pl.ds(y, 1), :]
        send_plane(ROOT, v_peers, v_send, v_recv)
        send_plane(ROOT + 1, [*v_peers, (gi, si)], d_send, d_recv)
        for d in range(DIRECT, NZ):
            remote(vbuf.at[own], vbuf.at[own], r_send, r_recv, z_peers[d - 1])
        for target in range(ROOT + 2, ROOT + DIRECT):
            send_plane(target, [*v_peers, (gi, si)], d_send, d_recv)

    @pl.when(z >= DIRECT)
    def _():
        row_moved.wait_recv()
        send_plane(z, v_peers, v_send, v_recv)

    count = jnp.full((1, LANE), jnp.sum(jnp.where(lane == si, count, 0.0)))
    z_moved.wait_recv()
    for j in range(NJ):
        top = zrecv[j, 0:1, :]
        for k in range(1, NZ):
            top = jnp.maximum(top, zrecv[k * NY + j, 0:1, :])
        first = jnp.zeros((1, LANE), jnp.float32)
        second = jnp.zeros((1, LANE), jnp.float32)
        for k in range(NZ):
            w = jnp.exp2((zrecv[k * NY + j, 0:1, :] - top) * LOG2E)
            first += w
            second += w * w * zrecv[k * NY + j, 1:2, :]
        shift = offset_buf[j : j + 1, :] - jnp.log(count)
        evidence_out[j : j + 1, :] = top + jnp.log(first) + shift
        ess_out[j : j + 1, :] = first * first / (second * count)

    @pl.when((z > ROOT) & (z < DIRECT))
    def _():
        moved(vbuf, d_send, d_recv).wait_recv()

    @pl.when((z == ROOT) | (z >= DIRECT))
    def _():
        v_moved.wait_recv()

    best = vbuf[0]
    for k in range(1, NG * NJ):
        best = jnp.maximum(best, vbuf[k])
    best = jnp.max(best)
    mass = jnp.zeros((1, LANE), jnp.float32)
    for k in range(NG * NJ):
        mass += jnp.exp2((vbuf[k] - best) * LOG2E)
    norm = best + jnp.log(jnp.full((1, LANE), jnp.sum(mass)))
    for j in range(NJ):
        posterior_out[j : j + 1, :] = vbuf[gi * NJ + j] - norm

    for copy in (id_moved, c_moved, z_moved, stats_moved(0), stats_moved(1)):
        copy.wait_send()

    @pl.when(z != ROOT)
    def _():
        moved(lse, l_send, l_recv).wait_send()

    @pl.when(z == ROOT)
    def _():
        moved(vbuf.at[pl.ds(0, NZ - DIRECT)], r_send, r_recv).wait_send()
        rows = zrecv.at[pl.ds(0, (DIRECT - 1) * NG * NJ // 2)]
        moved(rows, d_send, d_recv).wait_send()

    @pl.when((z == ROOT) | (z >= DIRECT))
    def _():
        v_moved.wait_send()


def finish(evidence, ess, posterior, evidence_out, ess_out, posterior_out, sem):
    pairs = ((evidence, evidence_out), (ess, ess_out), (posterior, posterior_out))
    copies = [pltpu.make_async_copy(a, b, sem.at[k]) for k, (a, b) in enumerate(pairs)]
    for copy in copies:
        copy.start()
    for copy in copies:
        copy.wait()


def body(summary, weight, offset, prior, event, live):
    rows, bins = summary.shape
    cols = weight.shape[1]
    dma, vmem, smem = pltpu.SemaphoreType.DMA, pltpu.VMEM, pltpu.SMEM
    f32 = jnp.float32
    hbm = pl.BlockSpec(memory_space=pltpu.HBM)
    local = pl.BlockSpec(memory_space=pltpu.VMEM)
    kept = vmem((NJ, LANE), f32)
    outs = pl.pallas_call(
        kernel,
        name="reweight",
        out_shape=(kept, kept, kept),
        in_specs=[hbm] * 6,
        out_specs=(local,) * 3,
        scratch_shapes=[
            vmem((rows, bins), jnp.bfloat16),
            vmem((bins, cols), jnp.bfloat16),
            vmem((2, max(SIZES), cols), f32),
            vmem((TILES, LANE), f32),
            vmem((NJ, LANE), f32),
            smem((TILES,), jnp.int32),
            smem((TILES,), jnp.int32),
            vmem((NY, TILES + 1, 1, LANE), f32),
            vmem((NJ, TILES, 2, LANE), f32),
            vmem((NY, TILES, 2, LANE), f32),
            vmem((3, EVENTS, LANE), f32),
            vmem((EVENTS, LANE), f32),
            vmem((NZ, EVENTS, LANE), f32),
            vmem((EVENTS, 2, LANE), f32),
            vmem((EVENTS, 2, LANE), f32),
            vmem((NZ, 1, LANE), f32),
            vmem((NG * NJ, 1, LANE), f32),
            dma((5,)),
            dma((len(SIZES),)),
            dma, dma,
            dma((2,)),
            dma((2,)),
            dma, dma, dma, dma, dma, dma, dma, dma, dma, dma, dma, dma,
            pltpu.SemaphoreType.REGULAR((2,)),
        ],
        compiler_params=pltpu.CompilerParams(
            collective_id=0, has_side_effects=True, vmem_limit_bytes=32 * 1024 * 1024
        ),
        cost_estimate=pl.CostEstimate(
            flops=2 * rows * bins * cols, bytes_accessed=2 * rows * bins, transcendentals=rows * cols
        ),
    )(*(
        pltpu.with_memory_space_constraint(a, pltpu.HBM)
        for a in (summary, weight, prior.reshape(TILES, LANE), offset.reshape(NJ, LANE), event, live)
    ))
    small = jax.ShapeDtypeStruct((NJ, LANE), f32)
    evidence, ess, posterior = pl.pallas_call(
        finish,
        name="finish",
        out_shape=(small, small, small),
        in_specs=[local] * 3,
        out_specs=(hbm,) * 3,
        scratch_shapes=[dma((3,))],
        compiler_params=pltpu.CompilerParams(vmem_limit_bytes=1024 * 1024),
    )(*outs)
    return evidence.reshape(1, cols), ess.reshape(1, cols), posterior.reshape(cols)


def solution(mesh):
    in_specs = (P("samp", None), P(None, "grid"), P("grid"), P("samp"), P("samp"), P("samp"))
    out_specs = (P("samp", "grid"), P("samp", "grid"), P("grid"))
    return jax.shard_map(body, mesh=mesh, in_specs=in_specs, out_specs=out_specs, check_vma=False)
```
